32 devices in a mesh: fy: 4 (over y, core), fx: 4 (over z), blk: 2 (over x).
Axes of the slice: x: 2, y: 2, z: 4, core: 2. Of those that a mesh axis runs over, the one named last changes fastest.
Arguments:
- sky_image: bfloat16 [8, 512, 512], P('blk', 'fy', 'fx'), may hold values from -33 to 33
- vis_data: bfloat16 [4, 4, 8, 2, 512], P('fy', 'fx', 'blk'), may hold values from -6 to 6
- interp_weights: bfloat16 [4, 4, 2, 4, 2, 128, 128], P('fy', 'fx'), may hold values from -0.25 to 0.25
- tile_rows: int32 [4, 4, 2, 4, 2], P('fy', 'fx'), may hold values from 0 to 127
- facet_list: int32 [4, 4, 2], P('fy', 'fx'), may hold values from 0 to 3, as said below
- vis_count: int32 [4, 4], P('fy', 'fx'), may hold values from 128 to 512
- wavelet_threshold: float32 [4, 8], P(None, 'blk'), may hold values from 0.05 to 0.5
- spectral_weight: float32 [], replicated, may hold values from 0.1 to 1
Outputs:
- restored: float32 [8, 512, 512], P('blk', 'fy', 'fx')
The draws below stay inside these ranges and needn't reach their ends.
Inputs may be any that keep to these rules, and one draw needn't show every extreme that they name: `facet_list`: the 2 facet numbers of one block are distinct.
All inputs are finite; a program needn't handle non-finite values.
Results may differ from the reference program's by a relative error of at most 0.0035.
Values may be sent and summed in bfloat16 or wider, within the bound.
A program may use at most 64 MiB of HBM per device.

```python
import math
import jax
import jax.numpy as jnp
from jax import lax

FACET = 128
CHANNELS = 8
TILE = 128
VT = 4
NNZ = 2
LEVELS = 4
NFY = 4
NFX = 4
FPB = 2
NY = 512
NX = 512
VIS = 512


def draw_sky_image(key, part):
    key_rows = jax.random.fold_in(key, 11)
    key_cols = jax.random.fold_in(key, 12)
    key_sky = jax.random.fold_in(key, 13)
    key_gain = jax.random.fold_in(key, 14)
    key_noise = jax.random.fold_in(key, 15)
    row_scale = jnp.exp(jax.random.uniform(key_rows, (NY, 1), jnp.float32) * math.log(3.2))
    col_scale = jnp.exp(jax.random.uniform(key_cols, (1, NX), jnp.float32) * math.log(3.2))
    sky_field = jnp.clip(jax.random.normal(key_sky, (NY, NX), jnp.float32), -4.0, 4.0)
    channel_gain = jax.random.uniform(key_gain, (CHANNELS, 1, 1), jnp.float32, 0.5, 1.5)
    channel_noise = 0.5 * jnp.clip(jax.random.normal(key_noise, (CHANNELS, NY, NX), jnp.float32), -4.0, 4.0)
    values = 0.5 * sky_field[None] * row_scale[None] * col_scale[None] * channel_gain + channel_noise
    return values.astype(jnp.bfloat16)


def draw_facet_list(key, part):
    keys_all = jax.random.split(jax.random.fold_in(key, 21), NFY * NFX)
    orders = jax.vmap(lambda block_key: jax.random.permutation(block_key, NFX))(keys_all)
    return orders[:, :FPB].reshape(NFY, NFX, FPB).astype(jnp.int32)


def touch_ends(array, own_key, smallest, largest):
    shape = array.shape
    index_at = [jax.random.randint(jax.random.fold_in(own_key, axis), (), 0, shape[axis]) for axis in range(len(shape))]
    array = array.at[tuple(index_at)].set(smallest)
    longest = shape.index(max(shape))
    index_at[longest] = (index_at[longest] + 1) % shape[longest]
    return array.at[tuple(index_at)].set(largest)


def block_levels(own_key, shape, cuts, least, top_value):
    loudness, own = 1.0, jax.random.fold_in(own_key, 6)
    for dim, blocks in cuts:
        draws = jnp.exp(jax.random.uniform(jax.random.fold_in(own, dim), (blocks,), jnp.float32, least / len(cuts), top_value / len(cuts)))
        loudness = loudness * jnp.repeat(draws, shape[dim] // blocks).reshape([-1 if axis == dim else 1 for axis in range(len(shape))])
    return loudness


def bell_draw(stream_key, extent, scale, bound, cuts=(), kind=jnp.bfloat16):
    factor_of = block_levels(stream_key, extent, cuts, -0.22, 0.18) if cuts else 1.0
    values = jax.random.normal(stream_key, extent, jnp.float32) * scale * factor_of
    return jnp.minimum(jnp.maximum(values, -bound), bound).astype(kind)


def setup_inputs(seed: int = 0) -> dict:
    streams_of = jax.random.split(jax.random.key(seed), 9)
    sky_image = draw_sky_image(jax.random.fold_in(streams_of[8], 71), 0)
    vis_data = bell_draw(streams_of[1], (NFY, NFX, CHANNELS, 2, VIS), 1.0, 6.0, ((0, 4), (1, 4), (2, 2)))
    interp_weights = bell_draw(streams_of[2], (NFY, NFX, FPB, VT, NNZ, TILE, FACET), (FPB * NNZ * FACET) ** -0.5, 0.25, ((0, 4), (1, 4)))
    tile_rows = touch_ends(jax.random.randint(streams_of[3], (NFY, NFX, FPB, VT, NNZ), 0, FACET), jax.random.fold_in(streams_of[3], 1), 0, FACET - 1).astype(jnp.int32)
    facet_list = draw_facet_list(jax.random.fold_in(streams_of[8], 71), 0)
    vis_count = touch_ends(jax.random.randint(streams_of[5], (NFY, NFX), VIS // 4, VIS + 1), jax.random.fold_in(streams_of[5], 1), VIS // 4, VIS).astype(jnp.int32)
    wavelet_threshold = jnp.clip(jnp.exp(math.log(0.5) - 2.3025851 * jax.random.uniform(streams_of[6], (LEVELS, CHANNELS), jnp.float32) ** block_levels(streams_of[6], (LEVELS, CHANNELS), ((1, 2),), -0.2, 0.2)), 0.05, 0.5)
    spectral_weight = jnp.clip(jnp.exp(jax.random.uniform(streams_of[7], (), jnp.float32, math.log(0.1), math.log(1.0))), 0.1, 1.0)
    return dict(sky_image=sky_image, vis_data=vis_data, interp_weights=interp_weights, tile_rows=tile_rows, facet_list=facet_list, vis_count=vis_count, wavelet_threshold=wavelet_threshold, spectral_weight=spectral_weight)


top_precision = lax.Precision.HIGHEST
descent_step = 2.0

def as_rounded(values):
    return lax.optimization_barrier(values.astype(jnp.bfloat16)).astype(jnp.float32)

def dft_tables(length):
    positions = jnp.arange(length, dtype=jnp.int32)
    phases = positions[:, None] * positions[None, :] % length
    angles = phases.astype(jnp.float32) * (2.0 * math.pi / length)
    scaling = 1.0 / math.sqrt(length)
    cosine = jnp.cos(angles) * scaling
    sinus_table = jnp.sin(angles) * scaling
    left_table = jnp.concatenate([cosine, -sinus_table], axis=0)
    right_table = jnp.stack([jnp.concatenate([cosine, -sinus_table], axis=1), jnp.concatenate([sinus_table, cosine], axis=1)])
    return (left_table, right_table)

def forward_transform(facets, left_table, right_table):
    halfway = jnp.einsum('wy,fcyx->fcwx', as_rounded(left_table), facets.astype(jnp.float32), precision=top_precision)
    halfway = as_rounded(halfway)
    facet_count, channel_count, doubled, facet_width = halfway.shape
    halfway = halfway.reshape(facet_count, channel_count, 2, doubled // 2, facet_width)
    spectra = jnp.einsum('fcpux,pxw->fcuw', halfway, as_rounded(right_table), precision=top_precision)
    return spectra.astype(jnp.bfloat16)

def adjoint_transform(spectrum_grad, left_table, right_table):
    halfway = jnp.einsum('fcuw,pxw->fcpux', spectrum_grad, right_table, precision=top_precision)
    facet_count, channel_count, parts_two, facet_width, other_width = halfway.shape
    halfway = halfway.reshape(facet_count, channel_count, 2 * facet_width, other_width)
    return jnp.einsum('wy,fcwx->fcyx', left_table, halfway, precision=top_precision)

def pick_rows(spectrum_one, row_ids):
    return jnp.take(spectrum_one, row_ids, axis=1)

def block_gradient(spectra, block_vis, block_weights, block_tiles, block_list, block_count):
    chosen = jnp.take(spectra, block_list, axis=0)
    picked = jax.vmap(pick_rows)(chosen, block_tiles)
    facet_count, channel_count, tile_count, slot_count, doubled = picked.shape
    picked = picked.reshape(facet_count, channel_count, tile_count, slot_count, 2, doubled // 2)
    weights_wide = block_weights.astype(jnp.float32)
    predicted = jnp.einsum('fanjv,fcanpv->cpaj', weights_wide, picked.astype(jnp.float32), precision=top_precision)
    predicted = predicted.reshape(channel_count, 2, -1)
    live_mask = jnp.arange(predicted.shape[2], dtype=jnp.int32) < block_count
    residual = jnp.where(live_mask, predicted - block_vis.astype(jnp.float32), 0.0)
    residual = as_rounded(residual).reshape(channel_count, 2, tile_count, -1)
    contrib = jnp.einsum('fanjv,cpaj->fancpv', weights_wide, residual, precision=top_precision)
    contrib = contrib.reshape(facet_count, tile_count, slot_count, channel_count, doubled)
    onehot = (block_tiles[..., None] == jnp.arange(doubled // 2, dtype=jnp.int32)).astype(jnp.float32)
    return jnp.einsum('fanu,fancw->fcuw', onehot, contrib, precision=top_precision)

def row_gradient(items):
    row_images, row_vis, row_weights, row_tiles, row_lists, row_counts = items
    left_table, right_table = dft_tables(FACET)
    spectra = forward_transform(row_images, left_table, right_table)
    block_grads = jax.vmap(block_gradient, in_axes=(None, 0, 0, 0, 0, 0))(spectra, row_vis, row_weights, row_tiles, row_lists, row_counts)
    flat_grads = block_grads.reshape((NFX * FPB,) + block_grads.shape[2:])
    row_total = jnp.zeros((NFX,) + block_grads.shape[2:], jnp.float32).at[row_lists.reshape(-1)].add(flat_grads)
    return adjoint_transform(row_total, left_table, right_table)

def smooth_axis(values, stride, axis_id):
    widths = [(0, 0), (0, 0), (0, 0)]
    widths[axis_id] = (stride, stride)
    padded = jnp.pad(values, widths)
    length = values.shape[axis_id]
    below_rows = lax.slice_in_dim(padded, 0, length, axis=axis_id)
    above_rows = lax.slice_in_dim(padded, 2 * stride, 2 * stride + length, axis=axis_id)
    return (below_rows + 2.0 * values + above_rows) * 0.25

def smooth_both(values, stride):
    return smooth_axis(smooth_axis(values, stride, 1), stride, 2)

def shrink_matrix(gram_matrix, offset):
    dimension = gram_matrix.shape[0]
    shifted = gram_matrix + offset * jnp.eye(dimension, dtype=jnp.float32)
    positions = jnp.arange(dimension, dtype=jnp.int32)
    columns = []
    for column_id in range(dimension):
        if column_id > 0:
            earlier = jnp.stack(columns, axis=1)
            correction = lax.optimization_barrier(jnp.sum(earlier * earlier[column_id][None, :], axis=1))
        else:
            correction = jnp.zeros((dimension,), jnp.float32)
        pivot = jnp.sqrt(shifted[column_id, column_id] - correction[column_id])
        column = (shifted[:, column_id] - correction) / pivot
        columns.append(jnp.where(positions >= column_id, column, 0.0))
    factor = jnp.stack(columns, axis=1)
    forward_rows = []
    for row_id in range(dimension):
        accum = gram_matrix[row_id]
        if row_id > 0:
            accum = accum - lax.optimization_barrier(jnp.sum(factor[row_id, :row_id][:, None] * jnp.stack(forward_rows, axis=0), axis=0))
        forward_rows.append(accum / factor[row_id, row_id])
    backward_rows = [None] * dimension
    for row_id in range(dimension - 1, -1, -1):
        accum = forward_rows[row_id]
        if row_id < dimension - 1:
            later = jnp.stack(backward_rows[row_id + 1:], axis=0)
            accum = accum - lax.optimization_barrier(jnp.sum(factor[row_id + 1:, row_id][:, None] * later, axis=0))
        backward_rows[row_id] = accum / factor[row_id, row_id]
    return jnp.stack(backward_rows, axis=0)

def reference(sky_image, vis_data, interp_weights, tile_rows, facet_list, vis_count, wavelet_threshold, spectral_weight):
    facets_all = sky_image.reshape(CHANNELS, NFY, FACET, NFX, FACET).transpose(1, 3, 0, 2, 4)
    gradient = lax.map(row_gradient, (facets_all, vis_data, interp_weights, tile_rows, facet_list, vis_count))
    gradient = gradient.transpose(2, 0, 3, 1, 4).reshape(CHANNELS, NY, NX)
    stepped = sky_image.astype(jnp.float32) - descent_step * gradient
    coarse = stepped
    clipped_sum = jnp.zeros_like(stepped)
    for level_index in range(LEVELS):
        smoother = smooth_both(coarse, 2 ** level_index)
        detail = coarse - smoother
        bound_now = wavelet_threshold[level_index][:, None, None]
        clipped_sum = clipped_sum + jnp.clip(detail, -bound_now, bound_now)
        coarse = smoother
    shrunk = stepped - clipped_sum
    blocks = shrunk.reshape(CHANNELS, NFY, FACET, NFX, FACET)
    grams = jnp.einsum('cyaxb,dyaxb->yxcd', blocks, blocks, precision=top_precision)
    offset = spectral_weight * (FACET * FACET)
    matrices = jax.vmap(jax.vmap(shrink_matrix, in_axes=(0, None)), in_axes=(0, None))(grams, offset)
    restored = jnp.einsum('cyaxb,yxcd->dyaxb', blocks, matrices, precision=top_precision)
    return restored.reshape(CHANNELS, NY, NX)
```

```python
import functools
import math

import jax
import jax.numpy as jnp
import numpy as np
from jax import lax
from jax.experimental import pallas as pl
from jax.experimental.pallas import tpu as pltpu
from jax.sharding import PartitionSpec as P

MESH = pl.DeviceIdType.MESH
descent_step = 2.0
f32, bf16 = jnp.float32, jnp.bfloat16


def dft_tables(length):
    positions = np.arange(length)
    angles = (positions[:, None] * positions[None, :] % length) * (2.0 * math.pi / length)
    scaling = 1.0 / math.sqrt(length)
    cosine, sinus = np.cos(angles) * scaling, np.sin(angles) * scaling
    left = np.concatenate([cosine, -sinus], axis=0)
    right = np.concatenate(
        [np.concatenate([cosine, -sinus], axis=1), np.concatenate([sinus, cosine], axis=1)], axis=0
    )
    return jnp.asarray(left.astype(np.float32), bf16), jnp.asarray(right.astype(np.float32), bf16)


def dot(a, b):
    return jnp.dot(a, b, preferred_element_type=f32)


def dot_nt(a, b):
    return lax.dot_general(a, b, (((1,), (1,)), ((), ())), preferred_element_type=f32)


def corners():
    return [(dy, dx) for dy in (-1, 0, 1) for dx in (-1, 0, 1) if (dy, dx) != (0, 0)]


def kernel(
    nfy, nfx, nblk, halo,
    rows_s, list_s, count_s, bound_s, weight_s,
    sky_h, vis_h, w_h, left_h, right_h,
    out_ref,
    sky, vis, w, left, right, vis8,
    oh_out, oh_in, pick_f, row_out, row_in, con_out, con_in, con_f,
    step_b, pack_l, pack_r, land_t, land_b, land_l, land_r,
    shr_b, shr_in,
    load_sem, oh_s, oh_r, row_s, row_r, con_s, con_r, halo_s, halo_r, blk_s, blk_r,
):
    fy, fx, bk = lax.axis_index("fy"), lax.axis_index("fx"), lax.axis_index("blk")
    _, _, facets, tiles, slots = rows_s.shape
    chans, size, _ = sky.shape
    rows = tiles * slots
    parts = 2 * chans

    loads = [
        pltpu.make_async_copy(src, dst, load_sem.at[i])
        for i, (src, dst) in enumerate(
            [(sky_h, sky), (left_h, left), (right_h, right), (vis_h, vis), (w_h, w)]
        )
    ]
    for load in loads:
        load.start()

    has = {-1: {0: fy > 0, 1: fx > 0}, 1: {0: fy < nfy - 1, 1: fx < nfx - 1}}

    def near(dy, dx):
        cond = None
        for d, axis in ((dy, 0), (dx, 1)):
            if d:
                cond = has[d][axis] if cond is None else jnp.logical_and(cond, has[d][axis])
        return cond

    barrier = pltpu.get_barrier_semaphore()
    for o in range(1, nfx):
        pl.semaphore_signal(
            barrier, inc=1, device_id=(fy, lax.rem(fx + o, nfx), bk), device_id_type=MESH
        )
    for o in range(1, nblk):
        pl.semaphore_signal(
            barrier, inc=1, device_id=(fy, fx, lax.rem(bk + o, nblk)), device_id_type=MESH
        )
    for dy, dx in corners():
        if dy:

            @pl.when(near(dy, dx))
            def _():
                pl.semaphore_signal(
                    barrier, inc=1, device_id=(fy + dy, fx + dx, bk), device_id_type=MESH
                )

    sub = lax.broadcasted_iota(jnp.int32, (rows, size), 0)
    lane = lax.broadcasted_iota(jnp.int32, (rows, size), 1)
    hots = []
    for f in range(facets):
        wanted = jnp.zeros((rows, size), jnp.int32)
        for a in range(tiles):
            for n in range(slots):
                wanted = jnp.where(sub == a * slots + n, rows_s[0, 0, f, a, n], wanted)
        hots.append(jnp.where(wanted == lane, 1.0, 0.0))

    def match(f, o):
        return (list_s[0, 0, f] == lax.rem(fx + o, nfx)).astype(f32)

    for o in range(nfx):
        hot = hots[0] * match(0, o)
        for f in range(1, facets):
            hot = hot + hots[f] * match(f, o)
        if o:
            oh_out[o - 1] = hot
        else:
            oh_in[0] = hot

    waits = 0
    for v in ((fy > 0), (fy < nfy - 1)):
        waits = waits + v.astype(jnp.int32)
    sides = 1 + (fx > 0).astype(jnp.int32) + (fx < nfx - 1).astype(jnp.int32)
    pl.semaphore_wait(barrier, nfx - 1 + nblk - 1 + waits * sides)

    def peer(src, dst, send, recv, o, way):
        target = lax.rem(fx + o, nfx) if way > 0 else lax.rem(fx + nfx - o, nfx)
        return pltpu.make_async_remote_copy(
            src_ref=src, dst_ref=dst, send_sem=send.at[o - 1], recv_sem=recv.at[o - 1],
            device_id=(fy, target, bk), device_id_type=MESH,
        )

    oh_copies = [
        peer(oh_out.at[o - 1], oh_in.at[o], oh_s, oh_r, o, 1) for o in range(1, nfx)
    ]
    for copy in oh_copies:
        copy.start()

    for load in loads[:3]:
        load.wait()
    specs = []
    for c in range(chans):
        half = dot(left[...], sky[c]).astype(bf16)
        half = jnp.concatenate([half[:size], half[size:]], axis=1)
        specs.append(dot(half, right[...]).astype(bf16))

    for copy in oh_copies:
        copy.wait_recv()
    hot = oh_in[...].reshape(nfx * rows, size).astype(bf16)
    for c in range(chans):
        picked = dot(hot, specs[c])
        for p in range(2):
            pick_f[pl.ds(2 * c + p, nfx * rows, stride=parts), :] = picked[
                :, p * size : (p + 1) * size
            ]
    flat = rows * parts
    row_in[0] = pick_f[0:flat].astype(bf16)
    row_copies = []
    for o in range(1, nfx):
        row_out[o - 1] = pick_f[o * flat : (o + 1) * flat].astype(bf16)
    for o in range(1, nfx):
        copy = peer(row_out.at[o - 1], row_in.at[o], row_s, row_r, o, -1)
        copy.start()
        row_copies.append(copy)

    adj = [
        dot_nt(left[p * size : (p + 1) * size], hot).astype(bf16) for p in range(2)
    ]
    for load in loads[3:]:
        load.wait()
    for c in range(chans):
        vis8[2 * c : 2 * c + 2, :] = vis[c].astype(f32)

    for copy in row_copies:
        copy.wait_recv()
    mine = []
    for f in range(facets):
        total = row_in[0].astype(f32) * match(f, 0)
        for o in range(1, nfx):
            total = total + row_in[o].astype(f32) * match(f, o)
        mine.append(total)
    live = count_s[0, 0]
    contrib = [[None] * rows for f in range(facets)]
    span = w.shape[3]
    for a in range(tiles):
        pred = -vis8[:, a * span : (a + 1) * span]
        for f in range(facets):
            for n in range(slots):
                at = a * slots + n
                row = mine[f][at * parts : (at + 1) * parts].astype(bf16)
                pred = pred + dot_nt(row, w[f, a, n])
        slot_id = lax.broadcasted_iota(jnp.int32, (parts, span), 1) + a * span
        residual = jnp.where(slot_id < live, pred, 0.0).astype(bf16)
        for f in range(facets):
            for n in range(slots):
                contrib[f][a * slots + n] = dot(residual, w[f, a, n])
    for o in range(nfx):
        for at in range(0, rows, 2):
            both = []
            for k in (at, at + 1):
                total = contrib[0][k] * match(0, o)
                for f in range(1, facets):
                    total = total + contrib[f][k] * match(f, o)
                both.append(total)
            value = jnp.concatenate(both, axis=0).astype(bf16)
            if o:
                con_out[o - 1, at * parts : (at + 2) * parts] = value
            else:
                con_in[0, at * parts : (at + 2) * parts] = value
    con_copies = []
    for o in range(1, nfx):
        copy = peer(con_out.at[o - 1], con_in.at[o], con_s, con_r, o, 1)
        copy.start()
        con_copies.append(copy)
    for copy in con_copies:
        copy.wait_recv()

    con_f[...] = con_in[...].reshape(nfx * flat, size).astype(f32)
    halves = []
    for c in range(chans):
        grad = jnp.concatenate(
            [con_f[pl.ds(2 * c + p, nfx * rows, stride=parts), :] for p in range(2)], axis=1
        ).astype(bf16)
        halves.append(dot_nt(grad, right[...]).astype(bf16))
    stepped = []
    for c in range(chans):
        grad = dot(adj[0], halves[c][:, :size]) + dot(adj[1], halves[c][:, size:])
        stepped.append(sky[c].astype(f32) - descent_step * grad)

    lane1 = lax.broadcasted_iota(jnp.int32, (size, size), 1)
    seg_l = seg_r = None
    for c in range(chans):
        step_b[c] = stepped[c].astype(bf16)
        to_l = stepped[c] if c == 0 else pltpu.roll(stepped[c], c * halo, 1)
        to_r = stepped[c] if c == 0 else pltpu.roll(stepped[c], size - c * halo, 1)
        seg_l = to_l if c == 0 else jnp.where(lane1 >= c * halo, to_l, seg_l)
        seg_r = to_r if c == 0 else jnp.where(lane1 < size - c * halo, to_r, seg_r)
    pack_l[...] = seg_l.astype(bf16)
    pack_r[...] = seg_r.astype(bf16)
    sources = {
        -1: {-1: pack_l.at[0:halo], 0: step_b.at[:, 0:halo], 1: pack_r.at[0:halo]},
        0: {-1: pack_l, 1: pack_r},
        1: {
            -1: pack_l.at[size - halo : size],
            0: step_b.at[:, size - halo : size],
            1: pack_r.at[size - halo : size],
        },
    }
    spot = {0: slice(0, size), -1: slice(size, size + halo), 1: slice(size + halo, size + 2 * halo)}

    def halo_copy(i, dy, dx):
        if dx == 0:
            dst = land_b if dy < 0 else land_t
        else:
            dst = (land_r if dx < 0 else land_l).at[spot[dy]]
        return pltpu.make_async_remote_copy(
            src_ref=sources[dy][dx], dst_ref=dst, send_sem=halo_s.at[i], recv_sem=halo_r.at[i],
            device_id=(fy + dy, fx + dx, bk), device_id_type=MESH,
        )

    for i, (dy, dx) in enumerate(corners()):

        @pl.when(near(dy, dx))
        def _():
            halo_copy(i, dy, dx).start()

    for i, (dy, dx) in enumerate(corners()):

        @pl.when(near(-dy, -dx))
        def _():
            halo_copy(i, dy, dx).wait_recv()

    tall = size + 2 * halo
    wide = 2 * size
    row_id = lax.broadcasted_iota(jnp.int32, (tall, wide), 0)
    col_id = lax.broadcasted_iota(jnp.int32, (tall, wide), 1)
    up, down, west, east = (
        halo * v.astype(jnp.int32) for v in (fy > 0, fy < nfy - 1, fx > 0, fx < nfx - 1)
    )
    inside = jnp.logical_and(
        jnp.logical_or(row_id < size + down, row_id >= tall - up),
        jnp.logical_or(col_id < size + east, col_id >= wide - west),
    )
    lane2 = lax.broadcasted_iota(jnp.int32, (tall, size), 1)
    from_l, from_r = land_l[...].astype(f32), land_r[...].astype(f32)
    levels = bound_s.shape[0]
    shrunk = []
    blk_copies = []
    for c in range(chans):
        own = jnp.concatenate(
            [stepped[c], land_b[c].astype(f32), land_t[c].astype(f32)], axis=0
        )
        right_part = from_r if c == 0 else pltpu.roll(from_r, size - c * halo, 1)
        left_part = from_l if c == 0 else pltpu.roll(from_l, c * halo, 1)
        beside = jnp.where(lane2 < size // 2, right_part, left_part)
        coarse = jnp.where(inside, jnp.concatenate([own, beside], axis=1), 0.0)
        clipped = None
        for level in range(levels):
            stride = 2**level
            smooth = (
                pltpu.roll(coarse, stride, 0) + 2.0 * coarse + pltpu.roll(coarse, tall - stride, 0)
            ) * 0.25
            smooth = (
                pltpu.roll(smooth, stride, 1) + 2.0 * smooth + pltpu.roll(smooth, wide - stride, 1)
            ) * 0.25
            bound = bound_s[level, c]
            detail = coarse[:size, :size] - smooth[:size, :size]
            detail = jnp.minimum(jnp.maximum(detail, -bound), bound)
            clipped = detail if level == 0 else clipped + detail
            if level < levels - 1:
                coarse = jnp.where(inside, smooth, 0.0)
        value = stepped[c] - clipped
        shrunk.append(value)
        shr_b[c] = value.astype(bf16)
        for o in range(1, nblk):
            copy = pltpu.make_async_remote_copy(
                src_ref=shr_b.at[c], dst_ref=shr_in.at[o - 1, c],
                send_sem=blk_s.at[o - 1, c], recv_sem=blk_r.at[o - 1, c],
                device_id=(fy, fx, lax.rem(bk + o, nblk)), device_id_type=MESH,
            )
            copy.start()
            blk_copies.append(copy)
    for copy in blk_copies:
        copy.wait_recv()
    everyone = list(shrunk)
    for o in range(1, nblk):
        for c in range(chans):
            everyone.append(shr_in[o - 1, c].astype(f32))

    total = len(everyone)
    part = {}
    for c in range(total):
        for d in range(c, total):
            prod = everyone[c] * everyone[d]
            part[c, d] = jnp.sum(prod, axis=0, keepdims=True)
    gram = []
    for c in range(total):
        line = jnp.concatenate([part[min(c, d), max(c, d)] for d in range(total)], axis=0)
        gram.append(jnp.broadcast_to(jnp.sum(line, axis=1, keepdims=True), (total, size)))
    offset = weight_s[0] * float(size * size)
    subs = lax.broadcasted_iota(jnp.int32, (total, size), 0)
    lhs = [g + jnp.where(subs == c, offset, 0.0) for c, g in enumerate(gram)]
    rhs = list(gram)

    def column(x, k):
        return jnp.broadcast_to(x[k : k + 1, :], (total, size))

    for k in range(total):
        inv = 1.0 / column(lhs[k], k)
        lhs[k] = lhs[k] * inv
        rhs[k] = rhs[k] * inv
        for i in range(total):
            if i != k:
                factor = column(lhs[i], k)
                lhs[i] = lhs[i] - factor * lhs[k]
                rhs[i] = rhs[i] - factor * rhs[k]
    for d in range(chans):
        acc = None
        for c in range(total):
            term = rhs[c][d : d + 1, :] * everyone[c]
            acc = term if acc is None else acc + term
        out_ref[d] = acc

    for copy in oh_copies + row_copies + con_copies + blk_copies:
        copy.wait_send()
    for i, (dy, dx) in enumerate(corners()):

        @pl.when(near(dy, dx))
        def _():
            halo_copy(i, dy, dx).wait_send()


def body(
    nfy, nfx, nblk,
    sky_image, vis_data, interp_weights, tile_rows, facet_list, vis_count,
    wavelet_threshold, spectral_weight,
):
    chans, size, _ = sky_image.shape
    facets, tiles, slots, span = interp_weights.shape[2:6]
    left, right = dft_tables(size)
    rows, parts = tiles * slots, 2 * chans
    flat = rows * parts
    halo = 2 ** wavelet_threshold.shape[0]
    tall = size + 2 * halo
    vmem = pltpu.VMEM
    dma = pltpu.SemaphoreType.DMA
    smem_spec = pl.BlockSpec(memory_space=pltpu.SMEM)
    any_spec = pl.BlockSpec(memory_space=pl.ANY)
    return pl.pallas_call(
        functools.partial(kernel, nfy, nfx, nblk, halo),
        out_shape=jax.ShapeDtypeStruct((chans, size, size), f32),
        in_specs=[smem_spec] * 5 + [any_spec] * 5,
        out_specs=pl.BlockSpec(memory_space=pltpu.VMEM),
        scratch_shapes=[
            vmem(sky_image.shape, bf16),
            vmem(vis_data.shape[2:], bf16),
            vmem(interp_weights.shape[2:], bf16),
            vmem(left.shape, bf16),
            vmem(right.shape, bf16),
            vmem((parts, vis_data.shape[4]), f32),
            vmem((nfx - 1, rows, size), f32),
            vmem((nfx, rows, size), f32),
            vmem((nfx * flat, size), f32),
            vmem((nfx - 1, flat, size), bf16),
            vmem((nfx, flat, size), bf16),
            vmem((nfx - 1, flat, size), bf16),
            vmem((nfx, flat, size), bf16),
            vmem((nfx * flat, size), f32),
            vmem((chans, size, size), bf16),
            vmem((size, size), bf16),
            vmem((size, size), bf16),
            vmem((chans, halo, size), bf16),
            vmem((chans, halo, size), bf16),
            vmem((tall, size), bf16),
            vmem((tall, size), bf16),
            vmem((chans, size, size), bf16),
            vmem((nblk - 1, chans, size, size), bf16),
            dma((5,)),
            dma((nfx - 1,)), dma((nfx - 1,)),
            dma((nfx - 1,)), dma((nfx - 1,)),
            dma((nfx - 1,)), dma((nfx - 1,)),
            dma((8,)), dma((8,)),
            dma((nblk - 1, chans)), dma((nblk - 1, chans)),
        ],
        compiler_params=pltpu.CompilerParams(collective_id=0, has_side_effects=True),
    )(
        tile_rows, facet_list, vis_count, wavelet_threshold, spectral_weight.reshape(1),
        sky_image, vis_data.reshape(vis_data.shape[2:]),
        interp_weights.reshape(interp_weights.shape[2:]), left, right,
    )


def solution(mesh):
    in_specs = (
        P("blk", "fy", "fx"),
        P("fy", "fx", "blk", None, None),
        P("fy", "fx", None, None, None, None, None),
        P("fy", "fx", None, None, None),
        P("fy", "fx", None),
        P("fy", "fx"),
        P(None, "blk"),
        P(),
    )
    out_specs = P("blk", "fy", "fx")
    step = functools.partial(body, mesh.shape["fy"], mesh.shape["fx"], mesh.shape["blk"])
    return jax.shard_map(step, mesh=mesh, in_specs=in_specs, out_specs=out_specs, check_vma=False)
```

```python
import functools
import math

import jax
import jax.numpy as jnp
import numpy as np
from jax import lax
from jax.experimental import pallas as pl
from jax.experimental.pallas import tpu as pltpu
from jax.sharding import PartitionSpec as P

MESH = pl.DeviceIdType.MESH
descent_step = 2.0
f32, bf16 = jnp.float32, jnp.bfloat16


def dft_tables(length):
    positions = np.arange(length)
    angles = (positions[:, None] * positions[None, :] % length) * (2.0 * math.pi / length)
    scaling = 1.0 / math.sqrt(length)
    cosine, sinus = np.cos(angles) * scaling, np.sin(angles) * scaling
    left = np.concatenate([cosine, -sinus], axis=0)
    right = np.concatenate(
        [np.concatenate([cosine, -sinus], axis=1), np.concatenate([sinus, cosine], axis=1)], axis=0
    )
    return jnp.asarray(left.astype(np.float32), bf16), jnp.asarray(right.astype(np.float32), bf16)


def smoothing_tables(size, halo, levels, chans):
    tall = size + 2 * halo
    gap = np.abs(np.arange(tall)[:, None] - np.arange(tall)[None, :])
    order = np.r_[halo:tall, 0:halo]
    row_all, col_all = [], []
    for before in (0, 1):
        for after in (0, 1):
            mask = np.r_[np.full(halo, before), np.ones(size), np.full(halo, after)]
            kept, lines = np.diag(mask), []
            for level in range(levels):
                smooth = 0.5 * (gap == 0) + 0.25 * (gap == 2**level)
                kept = mask[:, None] * (smooth @ kept)
                lines.append(kept[halo : halo + size][:, order])
            row_all.append(np.concatenate(lines, axis=0))
            col_all.append(np.concatenate([x[:, :size].T for x in lines], axis=1))
    beside = np.zeros((levels, size, chans, size))
    for level, x in enumerate(lines):
        for c in range(chans):
            beside[level, c * halo : (c + 1) * halo, c] = x[:, size : size + halo].T
            end = size - c * halo
            beside[level, end - halo : end, c] = x[:, size + halo :].T
    beside = beside.reshape(levels, size, chans * size)
    return [jnp.asarray(np.asarray(x, np.float32), bf16) for x in (row_all, col_all, beside)]


def dot(a, b):
    return jnp.dot(a, b, preferred_element_type=f32)


def dot_nt(a, b):
    return lax.dot_general(a, b, (((1,), (1,)), ((), ())), preferred_element_type=f32)


def corners():
    return [(dy, dx) for dy in (-1, 0, 1) for dx in (-1, 0, 1) if (dy, dx) != (0, 0)]


def kernel(
    nfy, nfx, nblk, halo,
    rows_s, list_s, count_s, bound_s, weight_s,
    sky_h, vis_h, w_h, left_h, right_h, rmat_h, cmat_h, beside_h,
    out_ref,
    sky, vis, w, left, right, rmat, cmat, beside, vis8,
    oh_out, oh_in, pick_f, row_out, row_in, con_out, con_in, con_f,
    step_b, pack_l, pack_r, land_t, land_b, land_l, land_r,
    shr_b, shr_in,
    load_sem, oh_s, oh_r, row_s, row_r, con_s, con_r, halo_s, halo_r, blk_s, blk_r,
):
    fy, fx, bk = lax.axis_index("fy"), lax.axis_index("fx"), lax.axis_index("blk")
    _, _, facets, slots, tiles = rows_s.shape
    chans, size, _ = sky.shape
    rows = tiles * slots
    parts = 2 * chans

    def edges(at, count):
        return 2 * (at > 0).astype(jnp.int32) + (at < count - 1).astype(jnp.int32)

    loads = [
        pltpu.make_async_copy(src, dst, load_sem.at[i])
        for i, (src, dst) in enumerate(
            [
                (sky_h, sky), (left_h, left), (right_h, right), (vis_h, vis), (w_h, w),
                (rmat_h.at[edges(fy, nfy)], rmat), (cmat_h.at[edges(fx, nfx)], cmat),
                (beside_h, beside),
            ]
        )
    ]
    for load in loads:
        load.start()

    for land in (land_t, land_b, land_l, land_r):
        land[...] = jnp.zeros(land.shape, bf16)

    has = {-1: {0: fy > 0, 1: fx > 0}, 1: {0: fy < nfy - 1, 1: fx < nfx - 1}}

    def near(dy, dx):
        cond = None
        for d, axis in ((dy, 0), (dx, 1)):
            if d:
                cond = has[d][axis] if cond is None else jnp.logical_and(cond, has[d][axis])
        return cond

    barrier = pltpu.get_barrier_semaphore()
    for o in range(1, nfx):
        pl.semaphore_signal(
            barrier, inc=1, device_id=(fy, lax.rem(fx + o, nfx), bk), device_id_type=MESH
        )
    for o in range(1, nblk):
        pl.semaphore_signal(
            barrier, inc=1, device_id=(fy, fx, lax.rem(bk + o, nblk)), device_id_type=MESH
        )
    for dy, dx in corners():
        if dy:

            @pl.when(near(dy, dx))
            def _():
                pl.semaphore_signal(
                    barrier, inc=1, device_id=(fy + dy, fx + dx, bk), device_id_type=MESH
                )

    sub = lax.broadcasted_iota(jnp.int32, (rows, size), 0)
    lane = lax.broadcasted_iota(jnp.int32, (rows, size), 1)
    hots = []
    for f in range(facets):
        wanted = jnp.zeros((rows, size), jnp.int32)
        for a in range(tiles):
            for n in range(slots):
                wanted = jnp.where(sub == a * slots + n, rows_s[0, 0, f, n, a], wanted)
        hots.append(jnp.where(wanted == lane, 1.0, 0.0))

    def match(f, o):
        return (list_s[0, 0, f] == lax.rem(fx + o, nfx)).astype(f32)

    for o in range(nfx):
        hot = hots[0] * match(0, o)
        for f in range(1, facets):
            hot = hot + hots[f] * match(f, o)
        if o:
            oh_out[o - 1] = hot
        else:
            oh_in[0] = hot

    waits = 0
    for v in ((fy > 0), (fy < nfy - 1)):
        waits = waits + v.astype(jnp.int32)
    sides = 1 + (fx > 0).astype(jnp.int32) + (fx < nfx - 1).astype(jnp.int32)
    pl.semaphore_wait(barrier, nfx - 1 + nblk - 1 + waits * sides)

    def peer(src, dst, send, recv, o, way):
        target = lax.rem(fx + o, nfx) if way > 0 else lax.rem(fx + nfx - o, nfx)
        return pltpu.make_async_remote_copy(
            src_ref=src, dst_ref=dst, send_sem=send.at[o - 1], recv_sem=recv.at[o - 1],
            device_id=(fy, target, bk), device_id_type=MESH,
        )

    oh_copies = [
        peer(oh_out.at[o - 1], oh_in.at[o], oh_s, oh_r, o, 1) for o in range(1, nfx)
    ]
    for copy in oh_copies:
        copy.start()

    for load in loads[:3]:
        load.wait()
    specs = []
    for c in range(chans):
        half = dot(left[...], sky[c]).astype(bf16)
        half = jnp.concatenate([half[:size], half[size:]], axis=1)
        specs.append(dot(half, right[...]).astype(bf16))

    for copy in oh_copies:
        copy.wait_recv()
    hot = oh_in[...].reshape(nfx * rows, size).astype(bf16)
    for c in range(chans):
        picked = dot(hot, specs[c])
        for p in range(2):
            pick_f[pl.ds(2 * c + p, nfx * rows, stride=parts), :] = picked[
                :, p * size : (p + 1) * size
            ]
    flat = rows * parts
    row_in[0] = pick_f[0:flat].astype(bf16)
    row_copies = []
    for o in range(1, nfx):
        row_out[o - 1] = pick_f[o * flat : (o + 1) * flat].astype(bf16)
    for o in range(1, nfx):
        copy = peer(row_out.at[o - 1], row_in.at[o], row_s, row_r, o, -1)
        copy.start()
        row_copies.append(copy)

    adj = [
        dot_nt(left[p * size : (p + 1) * size], hot).astype(bf16) for p in range(2)
    ]
    for load in loads[3:]:
        load.wait()
    for c in range(chans):
        vis8[2 * c : 2 * c + 2, :] = vis[c].astype(f32)

    for copy in row_copies:
        copy.wait_recv()
    mine = []
    for f in range(facets):
        total = row_in[0].astype(f32) * match(f, 0)
        for o in range(1, nfx):
            total = total + row_in[o].astype(f32) * match(f, o)
        mine.append(total)
    live = count_s[0, 0]
    contrib = [[None] * rows for f in range(facets)]
    span = w.shape[3]
    for a in range(tiles):
        pred = -vis8[:, a * span : (a + 1) * span]
        for f in range(facets):
            for n in range(slots):
                at = a * slots + n
                row = mine[f][at * parts : (at + 1) * parts].astype(bf16)
                pred = pred + dot_nt(row, w[f, a, n])
        slot_id = lax.broadcasted_iota(jnp.int32, (parts, span), 1) + a * span
        residual = jnp.where(slot_id < live, pred, 0.0).astype(bf16)
        for f in range(facets):
            for n in range(slots):
                contrib[f][a * slots + n] = dot(residual, w[f, a, n])
    for o in range(nfx):
        for at in range(0, rows, 2):
            both = []
            for k in (at, at + 1):
                total = contrib[0][k] * match(0, o)
                for f in range(1, facets):
                    total = total + contrib[f][k] * match(f, o)
                both.append(total)
            value = jnp.concatenate(both, axis=0).astype(bf16)
            if o:
                con_out[o - 1, at * parts : (at + 2) * parts] = value
            else:
                con_in[0, at * parts : (at + 2) * parts] = value
    con_copies = []
    for o in range(1, nfx):
        copy = peer(con_out.at[o - 1], con_in.at[o], con_s, con_r, o, 1)
        copy.start()
        con_copies.append(copy)
    for copy in con_copies:
        copy.wait_recv()

    con_f[...] = con_in[...].reshape(nfx * flat, size).astype(f32)
    halves = []
    for c in range(chans):
        grad = jnp.concatenate(
            [con_f[pl.ds(2 * c + p, nfx * rows, stride=parts), :] for p in range(2)], axis=1
        ).astype(bf16)
        halves.append(dot_nt(grad, right[...]).astype(bf16))
    stepped = []
    for c in range(chans):
        grad = dot(adj[0], halves[c][:, :size]) + dot(adj[1], halves[c][:, size:])
        stepped.append(sky[c].astype(f32) - descent_step * grad)

    lane1 = lax.broadcasted_iota(jnp.int32, (size, size), 1)
    seg_l = seg_r = None
    for c in range(chans):
        step_b[c] = stepped[c].astype(bf16)
        to_l = stepped[c] if c == 0 else pltpu.roll(stepped[c], c * halo, 1)
        to_r = stepped[c] if c == 0 else pltpu.roll(stepped[c], size - c * halo, 1)
        seg_l = to_l if c == 0 else jnp.where(lane1 >= c * halo, to_l, seg_l)
        seg_r = to_r if c == 0 else jnp.where(lane1 < size - c * halo, to_r, seg_r)
    pack_l[...] = seg_l.astype(bf16)
    pack_r[...] = seg_r.astype(bf16)
    sources = {
        -1: {-1: pack_l.at[0:halo], 0: step_b.at[:, 0:halo], 1: pack_r.at[0:halo]},
        0: {-1: pack_l, 1: pack_r},
        1: {
            -1: pack_l.at[size - halo : size],
            0: step_b.at[:, size - halo : size],
            1: pack_r.at[size - halo : size],
        },
    }
    spot = {0: slice(0, size), -1: slice(size, size + halo), 1: slice(size + halo, size + 2 * halo)}

    def halo_copy(i, dy, dx):
        if dx == 0:
            dst = land_b if dy < 0 else land_t
        else:
            dst = (land_r if dx < 0 else land_l).at[spot[dy]]
        return pltpu.make_async_remote_copy(
            src_ref=sources[dy][dx], dst_ref=dst, send_sem=halo_s.at[i], recv_sem=halo_r.at[i],
            device_id=(fy + dy, fx + dx, bk), device_id_type=MESH,
        )

    for i, (dy, dx) in enumerate(corners()):

        @pl.when(near(dy, dx))
        def _():
            halo_copy(i, dy, dx).start()

    for i, (dy, dx) in enumerate(corners()):

        @pl.when(near(-dy, -dx))
        def _():
            halo_copy(i, dy, dx).wait_recv()

    levels = bound_s.shape[0]
    side = lax.broadcasted_iota(jnp.int32, land_l.shape, 1)
    packed = jnp.where(
        side < size // 2, land_r[...].astype(f32), land_l[...].astype(f32)
    ).astype(bf16)
    across = dot(rmat[...], packed).astype(bf16)
    from_beside = [
        dot(across[l * size : (l + 1) * size], beside[l]) for l in range(levels)
    ]
    shrunk = []
    blk_copies = []
    for c in range(chans):
        if c % 2 == 0:
            pair = jnp.concatenate(
                [
                    jnp.concatenate([step_b[d], land_b[d], land_t[d]], axis=0)
                    for d in range(c, min(c + 2, chans))
                ],
                axis=1,
            )
            down = dot(rmat[...], pair).astype(bf16)
        at = (c % 2) * size
        coarse, clipped = stepped[c], None
        for l in range(levels):
            smooth = dot(
                down[l * size : (l + 1) * size, at : at + size],
                cmat[:, l * size : (l + 1) * size],
            )
            smooth = smooth + from_beside[l][:, c * size : (c + 1) * size]
            bound = bound_s[l, c]
            detail = jnp.minimum(jnp.maximum(coarse - smooth, -bound), bound)
            clipped = detail if l == 0 else clipped + detail
            coarse = smooth
        value = stepped[c] - clipped
        shrunk.append(value)
        shr_b[c] = value.astype(bf16)
        for o in range(1, nblk):
            copy = pltpu.make_async_remote_copy(
                src_ref=shr_b.at[c], dst_ref=shr_in.at[o - 1, c],
                send_sem=blk_s.at[o - 1, c], recv_sem=blk_r.at[o - 1, c],
                device_id=(fy, fx, lax.rem(bk + o, nblk)), device_id_type=MESH,
            )
            copy.start()
            blk_copies.append(copy)
    for copy in blk_copies:
        copy.wait_recv()
    everyone = list(shrunk)
    for o in range(1, nblk):
        for c in range(chans):
            everyone.append(shr_in[o - 1, c].astype(f32))

    total = len(everyone)
    part = {}
    for c in range(total):
        for d in range(c, total):
            prod = everyone[c] * everyone[d]
            part[c, d] = jnp.sum(prod, axis=0, keepdims=True)
    gram = []
    for c in range(total):
        line = jnp.concatenate([part[min(c, d), max(c, d)] for d in range(total)], axis=0)
        gram.append(jnp.broadcast_to(jnp.sum(line, axis=1, keepdims=True), (total, size)))
    offset = weight_s[0] * float(size * size)
    subs = lax.broadcasted_iota(jnp.int32, (total, size), 0)
    lhs = [g + jnp.where(subs == c, offset, 0.0) for c, g in enumerate(gram)]
    rhs = list(gram)

    def column(x, k):
        return jnp.broadcast_to(x[k : k + 1, :], (total, size))

    for k in range(total):
        inv = 1.0 / column(lhs[k], k)
        lhs[k] = lhs[k] * inv
        rhs[k] = rhs[k] * inv
        for i in range(total):
            if i != k:
                factor = column(lhs[i], k)
                lhs[i] = lhs[i] - factor * lhs[k]
                rhs[i] = rhs[i] - factor * rhs[k]
    for d in range(chans):
        acc = None
        for c in range(total):
            term = rhs[c][d : d + 1, :] * everyone[c]
            acc = term if acc is None else acc + term
        out_ref[d] = acc

    for copy in oh_copies + row_copies + con_copies + blk_copies:
        copy.wait_send()
    for i, (dy, dx) in enumerate(corners()):

        @pl.when(near(dy, dx))
        def _():
            halo_copy(i, dy, dx).wait_send()


def body(
    nfy, nfx, nblk,
    sky_image, vis_data, interp_weights, tile_rows, facet_list, vis_count,
    wavelet_threshold, spectral_weight,
):
    chans, size, _ = sky_image.shape
    facets, tiles, slots, span = interp_weights.shape[2:6]
    left, right = dft_tables(size)
    levels = wavelet_threshold.shape[0]
    rows, parts = tiles * slots, 2 * chans
    flat = rows * parts
    halo = 2**levels
    rmat, cmat, beside = smoothing_tables(size, halo, levels, chans)
    tall = size + 2 * halo
    vmem = pltpu.VMEM
    dma = pltpu.SemaphoreType.DMA
    smem_spec = pl.BlockSpec(memory_space=pltpu.SMEM)
    any_spec = pl.BlockSpec(memory_space=pl.ANY)
    return pl.pallas_call(
        functools.partial(kernel, nfy, nfx, nblk, halo),
        out_shape=jax.ShapeDtypeStruct((chans, size, size), f32),
        in_specs=[smem_spec] * 5 + [any_spec] * 8,
        out_specs=pl.BlockSpec(memory_space=pltpu.VMEM),
        scratch_shapes=[
            vmem(sky_image.shape, bf16),
            vmem(vis_data.shape[2:], bf16),
            vmem(interp_weights.shape[2:], bf16),
            vmem(left.shape, bf16),
            vmem(right.shape, bf16),
            vmem(rmat.shape[1:], bf16),
            vmem(cmat.shape[1:], bf16),
            vmem(beside.shape, bf16),
            vmem((parts, vis_data.shape[4]), f32),
            vmem((nfx - 1, rows, size), f32),
            vmem((nfx, rows, size), f32),
            vmem((nfx * flat, size), f32),
            vmem((nfx - 1, flat, size), bf16),
            vmem((nfx, flat, size), bf16),
            vmem((nfx - 1, flat, size), bf16),
            vmem((nfx, flat, size), bf16),
            vmem((nfx * flat, size), f32),
            vmem((chans, size, size), bf16),
            vmem((size, size), bf16),
            vmem((size, size), bf16),
            vmem((chans, halo, size), bf16),
            vmem((chans, halo, size), bf16),
            vmem((tall, size), bf16),
            vmem((tall, size), bf16),
            vmem((chans, size, size), bf16),
            vmem((nblk - 1, chans, size, size), bf16),
            dma((8,)),
            dma((nfx - 1,)), dma((nfx - 1,)),
            dma((nfx - 1,)), dma((nfx - 1,)),
            dma((nfx - 1,)), dma((nfx - 1,)),
            dma((8,)), dma((8,)),
            dma((nblk - 1, chans)), dma((nblk - 1, chans)),
        ],
        compiler_params=pltpu.CompilerParams(collective_id=0, has_side_effects=True),
    )(
        tile_rows.swapaxes(3, 4), facet_list, vis_count, wavelet_threshold, spectral_weight.reshape(1),
        sky_image, vis_data.reshape(vis_data.shape[2:]),
        interp_weights.reshape(interp_weights.shape[2:]), left, right,
        rmat, cmat, beside,
    )


def solution(mesh):
    in_specs = (
        P("blk", "fy", "fx"),
        P("fy", "fx", "blk", None, None),
        P("fy", "fx", None, None, None, None, None),
        P("fy", "fx", None, None, None),
        P("fy", "fx", None),
        P("fy", "fx"),
        P(None, "blk"),
        P(),
    )
    out_specs = P("blk", "fy", "fx")
    step = functools.partial(body, mesh.shape["fy"], mesh.shape["fx"], mesh.shape["blk"])
    return jax.shard_map(step, mesh=mesh, in_specs=in_specs, out_specs=out_specs, check_vma=False)
```

```python
import functools
import math

import jax
import jax.numpy as jnp
import numpy as np
from jax import lax
from jax.experimental import pallas as pl
from jax.experimental.pallas import tpu as pltpu
from jax.sharding import PartitionSpec as P

MESH = pl.DeviceIdType.MESH
descent_step = 2.0
f32, bf16 = jnp.float32, jnp.bfloat16


def dft_tables(length):
    positions = np.arange(length)
    angles = (positions[:, None] * positions[None, :] % length) * (2.0 * math.pi / length)
    scaling = 1.0 / math.sqrt(length)
    cosine, sinus = np.cos(angles) * scaling, np.sin(angles) * scaling
    left = np.concatenate([cosine, -sinus], axis=0)
    right = np.concatenate(
        [np.concatenate([cosine, -sinus], axis=1), np.concatenate([sinus, cosine], axis=1)], axis=0
    )
    return jnp.asarray(left.astype(np.float32), bf16), jnp.asarray(right.astype(np.float32), bf16)


def smoothing_tables(size, halo, levels, chans):
    tall = size + 2 * halo
    gap = np.abs(np.arange(tall)[:, None] - np.arange(tall)[None, :])
    order = np.r_[halo:tall, 0:halo]
    row_all, col_all = [], []
    for before in (0, 1):
        for after in (0, 1):
            mask = np.r_[np.full(halo, before), np.ones(size), np.full(halo, after)]
            kept, lines = np.diag(mask), []
            for level in range(levels):
                smooth = 0.5 * (gap == 0) + 0.25 * (gap == 2**level)
                kept = mask[:, None] * (smooth @ kept)
                lines.append(kept[halo : halo + size][:, order])
            row_all.append(np.concatenate(lines, axis=0))
            col_all.append(np.concatenate([x[:, :size].T for x in lines], axis=1))
    beside = np.zeros((levels, size, chans, size))
    for level, x in enumerate(lines):
        for c in range(chans):
            beside[level, c * halo : (c + 1) * halo, c] = x[:, size : size + halo].T
            end = size - c * halo
            beside[level, end - halo : end, c] = x[:, size + halo :].T
    beside = beside.reshape(levels, size, chans * size)
    rim = np.concatenate([np.r_[x[:halo], x[size - halo :]][:, size:] for x in lines], axis=0)
    return [jnp.asarray(np.asarray(x, np.float32), bf16) for x in (row_all, col_all, beside, rim)]


def dot(a, b):
    return jnp.dot(a, b, preferred_element_type=f32)


def dot_nt(a, b):
    return lax.dot_general(a, b, (((1,), (1,)), ((), ())), preferred_element_type=f32)


def corners():
    return [(dy, dx) for dy in (-1, 0, 1) for dx in (-1, 0, 1) if (dy, dx) != (0, 0)]


def kernel(
    nfy, nfx, nblk, halo,
    rows_s, list_s, count_s, bound_s, weight_s,
    sky_h, vis_h, w_h, left_h, right_h, rmat_h, cmat_h, beside_h, rim_h,
    out_ref,
    sky, vis, w, left, right, rmat, cmat, beside, rim, vis8,
    oh_out, oh_in, pick_f, row_out, row_in, con_out, con_in, con_f,
    step_b, pack_l, pack_r, land_t, land_b, land_l, land_r,
    shr_b, shr_in, edge_b, edge_in, side_b, side_in,
    load_sem, oh_s, oh_r, row_s, row_r, con_s, con_r, halo_s, halo_r, blk_s, blk_r,
):
    fy, fx, bk = lax.axis_index("fy"), lax.axis_index("fx"), lax.axis_index("blk")
    _, _, facets, slots, tiles = rows_s.shape
    chans, size, _ = sky.shape
    rows = tiles * slots
    parts = 2 * chans

    def edges(at, count):
        return 2 * (at > 0).astype(jnp.int32) + (at < count - 1).astype(jnp.int32)

    loads = [
        pltpu.make_async_copy(src, dst, load_sem.at[i])
        for i, (src, dst) in enumerate(
            [
                (sky_h, sky), (left_h, left), (right_h, right), (vis_h, vis), (w_h, w),
                (rmat_h.at[edges(fy, nfy)], rmat), (cmat_h.at[edges(fx, nfx)], cmat),
                (beside_h, beside), (rim_h, rim),
            ]
        )
    ]
    for load in loads:
        load.start()

    for land in (land_t, land_b, land_l, land_r):
        land[...] = jnp.zeros(land.shape, bf16)

    has = {-1: {0: fy > 0, 1: fx > 0}, 1: {0: fy < nfy - 1, 1: fx < nfx - 1}}

    def near(dy, dx):
        cond = None
        for d, axis in ((dy, 0), (dx, 1)):
            if d:
                cond = has[d][axis] if cond is None else jnp.logical_and(cond, has[d][axis])
        return cond

    barrier = pltpu.get_barrier_semaphore()
    for o in range(1, nfx):
        pl.semaphore_signal(
            barrier, inc=1, device_id=(fy, lax.rem(fx + o, nfx), bk), device_id_type=MESH
        )
    for o in range(1, nblk):
        pl.semaphore_signal(
            barrier, inc=1, device_id=(fy, fx, lax.rem(bk + o, nblk)), device_id_type=MESH
        )
    for dy, dx in corners():
        if dy:

            @pl.when(near(dy, dx))
            def _():
                pl.semaphore_signal(
                    barrier, inc=1, device_id=(fy + dy, fx + dx, bk), device_id_type=MESH
                )

    sub = lax.broadcasted_iota(jnp.int32, (rows, size), 0)
    lane = lax.broadcasted_iota(jnp.int32, (rows, size), 1)
    hots = []
    for f in range(facets):
        wanted = jnp.zeros((rows, size), jnp.int32)
        for a in range(tiles):
            for n in range(slots):
                wanted = jnp.where(sub == a * slots + n, rows_s[0, 0, f, n, a], wanted)
        hots.append(jnp.where(wanted == lane, 1.0, 0.0))

    def match(f, o):
        return (list_s[0, 0, f] == lax.rem(fx + o, nfx)).astype(f32)

    for o in range(nfx):
        hot = hots[0] * match(0, o)
        for f in range(1, facets):
            hot = hot + hots[f] * match(f, o)
        if o:
            oh_out[o - 1] = hot
        else:
            oh_in[0] = hot

    waits = 0
    for v in ((fy > 0), (fy < nfy - 1)):
        waits = waits + v.astype(jnp.int32)
    sides = 1 + (fx > 0).astype(jnp.int32) + (fx < nfx - 1).astype(jnp.int32)
    pl.semaphore_wait(barrier, nfx - 1 + nblk - 1 + waits * sides)

    def peer(src, dst, send, recv, o, way):
        target = lax.rem(fx + o, nfx) if way > 0 else lax.rem(fx + nfx - o, nfx)
        return pltpu.make_async_remote_copy(
            src_ref=src, dst_ref=dst, send_sem=send.at[o - 1], recv_sem=recv.at[o - 1],
            device_id=(fy, target, bk), device_id_type=MESH,
        )

    def start_all(copies, way):
        low = fx < nfx // 2

        @pl.when(low if way > 0 else jnp.logical_not(low))
        def _():
            for copy in reversed(copies):
                copy.start()

        @pl.when(jnp.logical_not(low) if way > 0 else low)
        def _():
            for copy in copies:
                copy.start()

    oh_copies = [
        peer(oh_out.at[o - 1], oh_in.at[o], oh_s, oh_r, o, 1) for o in range(1, nfx)
    ]
    start_all(oh_copies, 1)

    for load in loads[:3]:
        load.wait()
    specs = []
    for c in range(chans):
        half = dot(left[...], sky[c]).astype(bf16)
        half = jnp.concatenate([half[:size], half[size:]], axis=1)
        specs.append(dot(half, right[...]).astype(bf16))

    for copy in oh_copies:
        copy.wait_recv()
    hot = oh_in[...].reshape(nfx * rows, size).astype(bf16)
    for c in range(chans):
        picked = dot(hot, specs[c])
        for p in range(2):
            pick_f[pl.ds(2 * c + p, nfx * rows, stride=parts), :] = picked[
                :, p * size : (p + 1) * size
            ]
    flat = rows * parts
    row_in[0] = pick_f[0:flat].astype(bf16)
    row_copies = []
    for o in range(1, nfx):
        row_out[o - 1] = pick_f[o * flat : (o + 1) * flat].astype(bf16)
    for o in range(1, nfx):
        row_copies.append(peer(row_out.at[o - 1], row_in.at[o], row_s, row_r, o, -1))
    start_all(row_copies, -1)

    adj = [
        dot_nt(left[p * size : (p + 1) * size], hot).astype(bf16) for p in range(2)
    ]
    for load in loads[3:]:
        load.wait()
    for c in range(chans):
        vis8[2 * c : 2 * c + 2, :] = vis[c].astype(f32)

    for copy in row_copies:
        copy.wait_recv()
    mine = []
    for f in range(facets):
        total = row_in[0].astype(f32) * match(f, 0)
        for o in range(1, nfx):
            total = total + row_in[o].astype(f32) * match(f, o)
        mine.append(total)
    live = count_s[0, 0]
    contrib = [[None] * rows for f in range(facets)]
    span = w.shape[3]
    for a in range(tiles):
        pred = -vis8[:, a * span : (a + 1) * span]
        for f in range(facets):
            for n in range(slots):
                at = a * slots + n
                row = mine[f][at * parts : (at + 1) * parts].astype(bf16)
                pred = pred + dot_nt(row, w[f, a, n])
        slot_id = lax.broadcasted_iota(jnp.int32, (parts, span), 1) + a * span
        residual = jnp.where(slot_id < live, pred, 0.0).astype(bf16)
        for f in range(facets):
            for n in range(slots):
                contrib[f][a * slots + n] = dot(residual, w[f, a, n])
    for o in range(nfx):
        for at in range(0, rows, 2):
            both = []
            for k in (at, at + 1):
                total = contrib[0][k] * match(0, o)
                for f in range(1, facets):
                    total = total + contrib[f][k] * match(f, o)
                both.append(total)
            value = jnp.concatenate(both, axis=0).astype(bf16)
            if o:
                con_out[o - 1, at * parts : (at + 2) * parts] = value
            else:
                con_in[0, at * parts : (at + 2) * parts] = value
    con_copies = []
    for o in range(1, nfx):
        con_copies.append(peer(con_out.at[o - 1], con_in.at[o], con_s, con_r, o, 1))
    start_all(con_copies, 1)
    for copy in con_copies:
        copy.wait_recv()

    con_f[...] = con_in[...].reshape(nfx * flat, size).astype(f32)
    halves = []
    for c in range(chans):
        grad = jnp.concatenate(
            [con_f[pl.ds(2 * c + p, nfx * rows, stride=parts), :] for p in range(2)], axis=1
        ).astype(bf16)
        halves.append(dot_nt(grad, right[...]).astype(bf16))
    stepped = []
    for c in range(chans):
        grad = dot(adj[0], halves[c][:, :size]) + dot(adj[1], halves[c][:, size:])
        stepped.append(sky[c].astype(f32) - descent_step * grad)

    lane1 = lax.broadcasted_iota(jnp.int32, (size, size), 1)
    seg_l = seg_r = None
    for c in range(chans):
        step_b[c] = stepped[c].astype(bf16)
        to_l = stepped[c] if c == 0 else pltpu.roll(stepped[c], c * halo, 1)
        to_r = stepped[c] if c == 0 else pltpu.roll(stepped[c], size - c * halo, 1)
        seg_l = to_l if c == 0 else jnp.where(lane1 >= c * halo, to_l, seg_l)
        seg_r = to_r if c == 0 else jnp.where(lane1 < size - c * halo, to_r, seg_r)
    pack_l[...] = seg_l.astype(bf16)
    pack_r[...] = seg_r.astype(bf16)
    sources = {
        -1: {-1: pack_l.at[0:halo], 0: step_b.at[:, 0:halo], 1: pack_r.at[0:halo]},
        0: {-1: pack_l, 1: pack_r},
        1: {
            -1: pack_l.at[size - halo : size],
            0: step_b.at[:, size - halo : size],
            1: pack_r.at[size - halo : size],
        },
    }
    spot = {0: slice(0, size), -1: slice(size, size + halo), 1: slice(size + halo, size + 2 * halo)}

    def halo_copy(i, dy, dx):
        if dx == 0:
            dst = land_b if dy < 0 else land_t
        else:
            dst = (land_r if dx < 0 else land_l).at[spot[dy]]
        return pltpu.make_async_remote_copy(
            src_ref=sources[dy][dx], dst_ref=dst, send_sem=halo_s.at[i], recv_sem=halo_r.at[i],
            device_id=(fy + dy, fx + dx, bk), device_id_type=MESH,
        )

    for i, (dy, dx) in enumerate(corners()):

        @pl.when(near(dy, dx))
        def _():
            halo_copy(i, dy, dx).start()

    levels = bound_s.shape[0]
    inner = []
    for c in range(chans):
        if c % 2 == 0:
            pair = jnp.concatenate([step_b[d] for d in range(c, min(c + 2, chans))], axis=1)
            down = dot(rmat[:, :size], pair).astype(bf16)
        at = (c % 2) * size
        inner.append(
            [
                dot(
                    down[l * size : (l + 1) * size, at : at + size],
                    cmat[:, l * size : (l + 1) * size],
                )
                for l in range(levels)
            ]
        )

    def shrink(c, smooths):
        coarse, clipped = stepped[c], None
        for l, smooth in enumerate(smooths):
            bound = bound_s[l, c]
            detail = jnp.minimum(jnp.maximum(coarse - smooth, -bound), bound)
            clipped = detail if l == 0 else clipped + detail
            coarse = smooth
        return stepped[c] - clipped

    def across_blk(src, dst, i, o):
        return pltpu.make_async_remote_copy(
            src_ref=src, dst_ref=dst, send_sem=blk_s.at[o - 1, i], recv_sem=blk_r.at[o - 1, i],
            device_id=(fy, fx, lax.rem(bk + o, nblk)), device_id_type=MESH,
        )

    blk_copies = []
    for c in range(chans):
        shr_b[c] = shrink(c, inner[c])[halo : size - halo].astype(bf16)
        for o in range(1, nblk):
            blk_copies.append(across_blk(shr_b.at[c], shr_in.at[o - 1, c], c, o))
            blk_copies[-1].start()

    for i, (dy, dx) in enumerate(corners()):

        @pl.when(near(-dy, -dx))
        def _():
            halo_copy(i, dy, dx).wait_recv()

    side = lax.broadcasted_iota(jnp.int32, land_l.shape, 1)
    packed = jnp.where(
        side < size // 2, land_r[...].astype(f32), land_l[...].astype(f32)
    ).astype(bf16)
    across = dot(rmat[...], packed).astype(bf16)
    from_beside = [
        dot(across[l * size : (l + 1) * size], beside[l]) for l in range(levels)
    ]
    margin = jnp.concatenate(
        [jnp.concatenate([land_b[c], land_t[c]], axis=0) for c in range(chans)], axis=1
    )
    margin = dot(rim[...], margin).astype(bf16)
    two = 2 * halo
    from_rim = [
        dot(
            jnp.concatenate(
                [
                    margin[l * two : (l + 1) * two, c * size : (c + 1) * size]
                    for c in range(chans)
                ],
                axis=0,
            ),
            cmat[:, l * size : (l + 1) * size],
        )
        for l in range(levels)
    ]
    shrunk = []
    for c in range(chans):
        smooths = []
        for l in range(levels):
            smooth = inner[c][l] + from_beside[l][:, c * size : (c + 1) * size]
            top = smooth[:halo] + from_rim[l][c * two : c * two + halo]
            bottom = smooth[size - halo :] + from_rim[l][c * two + halo : (c + 1) * two]
            smooths.append(jnp.concatenate([top, smooth[halo : size - halo], bottom], axis=0))
        value = shrink(c, smooths)
        shrunk.append(value)
        edge_b[c] = jnp.concatenate([value[:halo], value[size - halo :]], axis=0).astype(bf16)
        turned = pltpu.roll(value[halo : size - halo], (halo + c * two) % size, 1)
        sides = turned if c == 0 else jnp.where(lane1[: size - two] >= c * two, turned, sides)
    side_b[...] = sides.astype(bf16)
    for o in range(1, nblk):
        blk_copies.append(across_blk(side_b, side_in.at[o - 1], chans, o))
        blk_copies[-1].start()
        blk_copies.append(across_blk(edge_b, edge_in.at[o - 1], chans + 1, o))
        blk_copies[-1].start()
    part = {}

    def products(those):
        for c, d in those:
            part[c, d] = jnp.sum(everyone[c] * everyone[d], axis=0, keepdims=True)

    everyone = list(shrunk)
    products([(c, d) for c in range(chans) for d in range(c, chans)])
    for copy in blk_copies:
        copy.wait_recv()
    brink = lax.broadcasted_iota(jnp.int32, (size - two, size), 1)
    brink = jnp.logical_or(brink < halo, brink >= size - halo)
    for o in range(1, nblk):
        sides = side_in[o - 1].astype(f32)
        for c in range(chans):
            edge = edge_in[o - 1, c].astype(f32)
            turned = pltpu.roll(sides, (2 * size - halo - c * two) % size, 1)
            middle = jnp.where(brink, turned, shr_in[o - 1, c].astype(f32))
            everyone.append(jnp.concatenate([edge[:halo], middle, edge[halo:]], axis=0))

    total = len(everyone)
    products([(c, d) for c in range(total) for d in range(max(c, chans), total)])
    gram = []
    for c in range(total):
        line = jnp.concatenate([part[min(c, d), max(c, d)] for d in range(total)], axis=0)
        gram.append(jnp.broadcast_to(jnp.sum(line, axis=1, keepdims=True), (total, size)))
    offset = weight_s[0] * float(size * size)
    subs = lax.broadcasted_iota(jnp.int32, (total, size), 0)
    lhs = [g + jnp.where(subs == c, offset, 0.0) for c, g in enumerate(gram)]
    rhs = list(gram)

    def column(x, k):
        return jnp.broadcast_to(x[k : k + 1, :], (total, size))

    for k in range(total):
        inv = 1.0 / column(lhs[k], k)
        lhs[k] = lhs[k] * inv
        rhs[k] = rhs[k] * inv
        for i in range(total):
            if i != k:
                factor = column(lhs[i], k)
                lhs[i] = lhs[i] - factor * lhs[k]
                rhs[i] = rhs[i] - factor * rhs[k]
    for d in range(chans):
        acc = None
        for c in range(total):
            term = rhs[c][d : d + 1, :] * everyone[c]
            acc = term if acc is None else acc + term
        out_ref[d] = acc

    for copy in oh_copies + row_copies + con_copies + blk_copies:
        copy.wait_send()
    for i, (dy, dx) in enumerate(corners()):

        @pl.when(near(dy, dx))
        def _():
            halo_copy(i, dy, dx).wait_send()


def body(
    nfy, nfx, nblk,
    sky_image, vis_data, interp_weights, tile_rows, facet_list, vis_count,
    wavelet_threshold, spectral_weight,
):
    chans, size, _ = sky_image.shape
    facets, tiles, slots, span = interp_weights.shape[2:6]
    left, right = dft_tables(size)
    levels = wavelet_threshold.shape[0]
    rows, parts = tiles * slots, 2 * chans
    flat = rows * parts
    halo = 2**levels
    rmat, cmat, beside, rim = smoothing_tables(size, halo, levels, chans)
    tall = size + 2 * halo
    vmem = pltpu.VMEM
    dma = pltpu.SemaphoreType.DMA
    smem_spec = pl.BlockSpec(memory_space=pltpu.SMEM)
    any_spec = pl.BlockSpec(memory_space=pl.ANY)
    return pl.pallas_call(
        functools.partial(kernel, nfy, nfx, nblk, halo),
        out_shape=pltpu.VMEM((chans, size, size), f32),
        in_specs=[smem_spec] * 5 + [any_spec] * 9,
        out_specs=pl.BlockSpec(memory_space=pltpu.VMEM),
        scratch_shapes=[
            vmem(sky_image.shape, bf16),
            vmem(vis_data.shape[2:], bf16),
            vmem(interp_weights.shape[2:], bf16),
            vmem(left.shape, bf16),
            vmem(right.shape, bf16),
            vmem(rmat.shape[1:], bf16),
            vmem(cmat.shape[1:], bf16),
            vmem(beside.shape, bf16),
            vmem(rim.shape, bf16),
            vmem((parts, vis_data.shape[4]), f32),
            vmem((nfx - 1, rows, size), f32),
            vmem((nfx, rows, size), f32),
            vmem((nfx * flat, size), f32),
            vmem((nfx - 1, flat, size), bf16),
            vmem((nfx, flat, size), bf16),
            vmem((nfx - 1, flat, size), bf16),
            vmem((nfx, flat, size), bf16),
            vmem((nfx * flat, size), f32),
            vmem((chans, size, size), bf16),
            vmem((size, size), bf16),
            vmem((size, size), bf16),
            vmem((chans, halo, size), bf16),
            vmem((chans, halo, size), bf16),
            vmem((tall, size), bf16),
            vmem((tall, size), bf16),
            vmem((chans, size - 2 * halo, size), bf16),
            vmem((nblk - 1, chans, size - 2 * halo, size), bf16),
            vmem((chans, 2 * halo, size), bf16),
            vmem((nblk - 1, chans, 2 * halo, size), bf16),
            vmem((size - 2 * halo, size), bf16),
            vmem((nblk - 1, size - 2 * halo, size), bf16),
            dma((9,)),
            dma((nfx - 1,)), dma((nfx - 1,)),
            dma((nfx - 1,)), dma((nfx - 1,)),
            dma((nfx - 1,)), dma((nfx - 1,)),
            dma((8,)), dma((8,)),
            dma((nblk - 1, chans + 2)), dma((nblk - 1, chans + 2)),
        ],
        compiler_params=pltpu.CompilerParams(collective_id=0, has_side_effects=True),
    )(
        tile_rows.swapaxes(3, 4), facet_list, vis_count, wavelet_threshold, spectral_weight.reshape(1),
        sky_image, vis_data.reshape(vis_data.shape[2:]),
        interp_weights.reshape(interp_weights.shape[2:]), left, right,
        rmat, cmat, beside, rim,
    )


def solution(mesh):
    in_specs = (
        P("blk", "fy", "fx"),
        P("fy", "fx", "blk", None, None),
        P("fy", "fx", None, None, None, None, None),
        P("fy", "fx", None, None, None),
        P("fy", "fx", None),
        P("fy", "fx"),
        P(None, "blk"),
        P(),
    )
    out_specs = P("blk", "fy", "fx")
    step = functools.partial(body, mesh.shape["fy"], mesh.shape["fx"], mesh.shape["blk"])
    return jax.shard_map(step, mesh=mesh, in_specs=in_specs, out_specs=out_specs, check_vma=False)
```

```python
import functools
import math

import jax
import jax.numpy as jnp
import numpy as np
from jax import lax
from jax.experimental import pallas as pl
from jax.experimental.pallas import tpu as pltpu
from jax.sharding import PartitionSpec as P

MESH = pl.DeviceIdType.MESH
descent_step = 2.0
f32, bf16 = jnp.float32, jnp.bfloat16


def dft_tables(length):
    positions = np.arange(length)
    angles = (positions[:, None] * positions[None, :] % length) * (2.0 * math.pi / length)
    scaling = 1.0 / math.sqrt(length)
    cosine, sinus = np.cos(angles) * scaling, np.sin(angles) * scaling
    left = np.concatenate([cosine, -sinus], axis=0)
    right = np.concatenate(
        [np.concatenate([cosine, -sinus], axis=1), np.concatenate([sinus, cosine], axis=1)], axis=0
    )
    return jnp.asarray(left.astype(np.float32), bf16), jnp.asarray(right.astype(np.float32), bf16)


def smoothing_tables(size, halo, levels, chans):
    tall = size + 2 * halo
    gap = np.abs(np.arange(tall)[:, None] - np.arange(tall)[None, :])
    order = np.r_[halo:tall, 0:halo]
    row_all, col_all = [], []
    for before in (0, 1):
        for after in (0, 1):
            mask = np.r_[np.full(halo, before), np.ones(size), np.full(halo, after)]
            kept, lines = np.diag(mask), []
            for level in range(levels):
                smooth = 0.5 * (gap == 0) + 0.25 * (gap == 2**level)
                kept = mask[:, None] * (smooth @ kept)
                lines.append(kept[halo : halo + size][:, order])
            row_all.append(np.concatenate(lines, axis=0))
            col_all.append(np.concatenate([x[:, :size].T for x in lines], axis=1))
    beside = np.zeros((levels, size, chans, size))
    for level, x in enumerate(lines):
        for c in range(chans):
            beside[level, c * halo : (c + 1) * halo, c] = x[:, size : size + halo].T
            end = size - c * halo
            beside[level, end - halo : end, c] = x[:, size + halo :].T
    beside = beside.reshape(levels, size, chans * size)
    rim = np.concatenate([np.r_[x[:halo], x[size - halo :]][:, size:] for x in lines], axis=0)
    return [jnp.asarray(np.asarray(x, np.float32), bf16) for x in (row_all, col_all, beside, rim)]


def dot(a, b):
    return jnp.dot(a, b, preferred_element_type=f32)


def dot_nt(a, b):
    return lax.dot_general(a, b, (((1,), (1,)), ((), ())), preferred_element_type=f32)


def corners():
    return [(dy, dx) for dy in (-1, 0, 1) for dx in (-1, 0, 1) if (dy, dx) != (0, 0)]


def kernel(
    nfy, nfx, nblk, halo,
    rows_h, list_h, count_h, bound_h, weight_h, sky_h, vis_h, w_h, left_h, right_h, rmat_h, cmat_h, beside_h, rim_h,
    out_ref,
    rows_s, list_s, count_s, bound_s, weight_s,
    sky, vis, w, left, right, rmat, cmat, beside, rim, vis8,
    oh_out, oh_in, pick_f, row_out, row_in, con_out, con_in, con_f,
    step_b, pack_l, pack_r, land_t, land_b, land_l, land_r,
    shr_b, shr_in, edge_b, edge_in, side_b, side_in,
    load_sem, small_sem, oh_s, oh_r, row_s, row_r, con_s, con_r, halo_s, halo_r, blk_s, blk_r,
):
    fy, fx, bk = lax.axis_index("fy"), lax.axis_index("fx"), lax.axis_index("blk")
    _, _, facets, slots, tiles = rows_s.shape
    chans, size, _ = sky.shape
    rows = tiles * slots
    parts = 2 * chans

    small = [
        pltpu.make_async_copy(src, dst, small_sem.at[i])
        for i, (src, dst) in enumerate(
            [
                (rows_h, rows_s), (list_h, list_s), (count_h, count_s), (bound_h, bound_s),
                (weight_h, weight_s),
            ]
        )
    ]
    for load in small:
        load.start()

    for land in (land_t, land_b, land_l, land_r):
        land[...] = jnp.zeros(land.shape, bf16)

    has = {-1: {0: fy > 0, 1: fx > 0}, 1: {0: fy < nfy - 1, 1: fx < nfx - 1}}

    def near(dy, dx):
        cond = None
        for d, axis in ((dy, 0), (dx, 1)):
            if d:
                cond = has[d][axis] if cond is None else jnp.logical_and(cond, has[d][axis])
        return cond

    barrier = pltpu.get_barrier_semaphore()
    for o in range(1, nfx):
        pl.semaphore_signal(
            barrier, inc=1, device_id=(fy, lax.rem(fx + o, nfx), bk), device_id_type=MESH
        )
    for o in range(1, nblk):
        pl.semaphore_signal(
            barrier, inc=1, device_id=(fy, fx, lax.rem(bk + o, nblk)), device_id_type=MESH
        )
    for dy, dx in corners():
        if dy:

            @pl.when(near(dy, dx))
            def _():
                pl.semaphore_signal(
                    barrier, inc=1, device_id=(fy + dy, fx + dx, bk), device_id_type=MESH
                )

    def edges(at, count):
        return 2 * (at > 0).astype(jnp.int32) + (at < count - 1).astype(jnp.int32)

    loads = [
        pltpu.make_async_copy(src, dst, load_sem.at[i])
        for i, (src, dst) in enumerate(
            [
                (sky_h, sky), (left_h, left), (right_h, right), (vis_h, vis), (w_h, w),
                (rmat_h.at[edges(fy, nfy)], rmat), (cmat_h.at[edges(fx, nfx)], cmat),
                (beside_h, beside), (rim_h, rim),
            ]
        )
    ]
    for load in loads:
        load.start()

    for load in small:
        load.wait()

    sub = lax.broadcasted_iota(jnp.int32, (rows, size), 0)
    lane = lax.broadcasted_iota(jnp.int32, (rows, size), 1)
    hots = []
    for f in range(facets):
        wanted = jnp.zeros((rows, size), jnp.int32)
        for a in range(tiles):
            for n in range(slots):
                wanted = jnp.where(sub == a * slots + n, rows_s[0, 0, f, n, a], wanted)
        hots.append(jnp.where(wanted == lane, 1.0, 0.0))

    def match(f, o):
        return (list_s[0, 0, f] == lax.rem(fx + o, nfx)).astype(f32)

    for o in range(nfx):
        hot = hots[0] * match(0, o)
        for f in range(1, facets):
            hot = hot + hots[f] * match(f, o)
        if o:
            oh_out[o - 1] = hot
        else:
            oh_in[0] = hot

    waits = 0
    for v in ((fy > 0), (fy < nfy - 1)):
        waits = waits + v.astype(jnp.int32)
    sides = 1 + (fx > 0).astype(jnp.int32) + (fx < nfx - 1).astype(jnp.int32)
    pl.semaphore_wait(barrier, nfx - 1 + nblk - 1 + waits * sides)

    def peer(src, dst, send, recv, o, way):
        target = lax.rem(fx + o, nfx) if way > 0 else lax.rem(fx + nfx - o, nfx)
        return pltpu.make_async_remote_copy(
            src_ref=src, dst_ref=dst, send_sem=send.at[o - 1], recv_sem=recv.at[o - 1],
            device_id=(fy, target, bk), device_id_type=MESH,
        )

    def start_all(copies, way):
        low = fx < nfx // 2

        @pl.when(low if way > 0 else jnp.logical_not(low))
        def _():
            for copy in reversed(copies):
                copy.start()

        @pl.when(jnp.logical_not(low) if way > 0 else low)
        def _():
            for copy in copies:
                copy.start()

    oh_copies = [
        peer(oh_out.at[o - 1], oh_in.at[o], oh_s, oh_r, o, 1) for o in range(1, nfx)
    ]
    start_all(oh_copies, 1)

    for load in loads[:3]:
        load.wait()
    specs = []
    for c in range(chans):
        half = dot(left[...], sky[c]).astype(bf16)
        half = jnp.concatenate([half[:size], half[size:]], axis=1)
        specs.append(dot(half, right[...]).astype(bf16))

    for copy in oh_copies:
        copy.wait_recv()
    hot = oh_in[...].reshape(nfx * rows, size).astype(bf16)
    for c in range(chans):
        picked = dot(hot, specs[c])
        for p in range(2):
            pick_f[pl.ds(2 * c + p, nfx * rows, stride=parts), :] = picked[
                :, p * size : (p + 1) * size
            ]
    flat = rows * parts
    row_in[0] = pick_f[0:flat].astype(bf16)
    row_copies = []
    for o in range(1, nfx):
        row_out[o - 1] = pick_f[o * flat : (o + 1) * flat].astype(bf16)
    for o in range(1, nfx):
        row_copies.append(peer(row_out.at[o - 1], row_in.at[o], row_s, row_r, o, -1))
    start_all(row_copies, -1)

    adj = [
        dot_nt(left[p * size : (p + 1) * size], hot).astype(bf16) for p in range(2)
    ]
    for load in loads[3:]:
        load.wait()
    for c in range(chans):
        vis8[2 * c : 2 * c + 2, :] = vis[c].astype(f32)

    for copy in row_copies:
        copy.wait_recv()
    mine = []
    for f in range(facets):
        total = row_in[0].astype(f32) * match(f, 0)
        for o in range(1, nfx):
            total = total + row_in[o].astype(f32) * match(f, o)
        mine.append(total)
    live = count_s[0, 0]
    contrib = [[None] * rows for f in range(facets)]
    span = w.shape[3]
    for a in range(tiles):
        pred = -vis8[:, a * span : (a + 1) * span]
        for f in range(facets):
            for n in range(slots):
                at = a * slots + n
                row = mine[f][at * parts : (at + 1) * parts].astype(bf16)
                pred = pred + dot_nt(row, w[f, a, n])
        slot_id = lax.broadcasted_iota(jnp.int32, (parts, span), 1) + a * span
        residual = jnp.where(slot_id < live, pred, 0.0).astype(bf16)
        for f in range(facets):
            for n in range(slots):
                contrib[f][a * slots + n] = dot(residual, w[f, a, n])
    for o in range(nfx):
        for at in range(0, rows, 2):
            both = []
            for k in (at, at + 1):
                total = contrib[0][k] * match(0, o)
                for f in range(1, facets):
                    total = total + contrib[f][k] * match(f, o)
                both.append(total)
            value = jnp.concatenate(both, axis=0).astype(bf16)
            if o:
                con_out[o - 1, at * parts : (at + 2) * parts] = value
            else:
                con_in[0, at * parts : (at + 2) * parts] = value
    con_copies = []
    for o in range(1, nfx):
        con_copies.append(peer(con_out.at[o - 1], con_in.at[o], con_s, con_r, o, 1))
    start_all(con_copies, 1)
    for copy in con_copies:
        copy.wait_recv()

    con_f[...] = con_in[...].reshape(nfx * flat, size).astype(f32)
    halves = []
    for c in range(chans):
        grad = jnp.concatenate(
            [con_f[pl.ds(2 * c + p, nfx * rows, stride=parts), :] for p in range(2)], axis=1
        ).astype(bf16)
        halves.append(dot_nt(grad, right[...]).astype(bf16))
    stepped = []
    for c in range(chans):
        grad = dot(adj[0], halves[c][:, :size]) + dot(adj[1], halves[c][:, size:])
        stepped.append(sky[c].astype(f32) - descent_step * grad)

    lane1 = lax.broadcasted_iota(jnp.int32, (size, size), 1)
    seg_l = seg_r = None
    for c in range(chans):
        step_b[c] = stepped[c].astype(bf16)
        to_l = stepped[c] if c == 0 else pltpu.roll(stepped[c], c * halo, 1)
        to_r = stepped[c] if c == 0 else pltpu.roll(stepped[c], size - c * halo, 1)
        seg_l = to_l if c == 0 else jnp.where(lane1 >= c * halo, to_l, seg_l)
        seg_r = to_r if c == 0 else jnp.where(lane1 < size - c * halo, to_r, seg_r)
    pack_l[...] = seg_l.astype(bf16)
    pack_r[...] = seg_r.astype(bf16)
    sources = {
        -1: {-1: pack_l.at[0:halo], 0: step_b.at[:, 0:halo], 1: pack_r.at[0:halo]},
        0: {-1: pack_l, 1: pack_r},
        1: {
            -1: pack_l.at[size - halo : size],
            0: step_b.at[:, size - halo : size],
            1: pack_r.at[size - halo : size],
        },
    }
    spot = {0: slice(0, size), -1: slice(size, size + halo), 1: slice(size + halo, size + 2 * halo)}

    def halo_copy(i, dy, dx):
        if dx == 0:
            dst = land_b if dy < 0 else land_t
        else:
            dst = (land_r if dx < 0 else land_l).at[spot[dy]]
        return pltpu.make_async_remote_copy(
            src_ref=sources[dy][dx], dst_ref=dst, send_sem=halo_s.at[i], recv_sem=halo_r.at[i],
            device_id=(fy + dy, fx + dx, bk), device_id_type=MESH,
        )

    for i, (dy, dx) in enumerate(corners()):

        @pl.when(near(dy, dx))
        def _():
            halo_copy(i, dy, dx).start()

    levels = bound_s.shape[0]
    inner = []
    for c in range(chans):
        if c % 2 == 0:
            pair = jnp.concatenate([step_b[d] for d in range(c, min(c + 2, chans))], axis=1)
            down = dot(rmat[:, :size], pair).astype(bf16)
        at = (c % 2) * size
        inner.append(
            [
                dot(
                    down[l * size : (l + 1) * size, at : at + size],
                    cmat[:, l * size : (l + 1) * size],
                )
                for l in range(levels)
            ]
        )

    def shrink(c, smooths):
        coarse, clipped = stepped[c], None
        for l, smooth in enumerate(smooths):
            bound = bound_s[l, c]
            detail = jnp.minimum(jnp.maximum(coarse - smooth, -bound), bound)
            clipped = detail if l == 0 else clipped + detail
            coarse = smooth
        return stepped[c] - clipped

    def across_blk(src, dst, i, o):
        return pltpu.make_async_remote_copy(
            src_ref=src, dst_ref=dst, send_sem=blk_s.at[o - 1, i], recv_sem=blk_r.at[o - 1, i],
            device_id=(fy, fx, lax.rem(bk + o, nblk)), device_id_type=MESH,
        )

    blk_copies = []
    for c in range(chans):
        shr_b[c] = shrink(c, inner[c])[halo : size - halo].astype(bf16)
        for o in range(1, nblk):
            blk_copies.append(across_blk(shr_b.at[c], shr_in.at[o - 1, c], c, o))
            blk_copies[-1].start()

    for i, (dy, dx) in enumerate(corners()):

        @pl.when(near(-dy, -dx))
        def _():
            halo_copy(i, dy, dx).wait_recv()

    side = lax.broadcasted_iota(jnp.int32, land_l.shape, 1)
    packed = jnp.where(
        side < size // 2, land_r[...].astype(f32), land_l[...].astype(f32)
    ).astype(bf16)
    across = dot(rmat[...], packed).astype(bf16)
    from_beside = [
        dot(across[l * size : (l + 1) * size], beside[l]) for l in range(levels)
    ]
    margin = jnp.concatenate(
        [jnp.concatenate([land_b[c], land_t[c]], axis=0) for c in range(chans)], axis=1
    )
    margin = dot(rim[...], margin).astype(bf16)
    two = 2 * halo
    from_rim = [
        dot(
            jnp.concatenate(
                [
                    margin[l * two : (l + 1) * two, c * size : (c + 1) * size]
                    for c in range(chans)
                ],
                axis=0,
            ),
            cmat[:, l * size : (l + 1) * size],
        )
        for l in range(levels)
    ]
    shrunk = []
    for c in range(chans):
        smooths = []
        for l in range(levels):
            smooth = inner[c][l] + from_beside[l][:, c * size : (c + 1) * size]
            top = smooth[:halo] + from_rim[l][c * two : c * two + halo]
            bottom = smooth[size - halo :] + from_rim[l][c * two + halo : (c + 1) * two]
            smooths.append(jnp.concatenate([top, smooth[halo : size - halo], bottom], axis=0))
        value = shrink(c, smooths)
        shrunk.append(value)
        edge_b[c] = jnp.concatenate([value[:halo], value[size - halo :]], axis=0).astype(bf16)
        turned = pltpu.roll(value[halo : size - halo], (halo + c * two) % size, 1)
        sides = turned if c == 0 else jnp.where(lane1[: size - two] >= c * two, turned, sides)
    side_b[...] = sides.astype(bf16)
    for o in range(1, nblk):
        blk_copies.append(across_blk(side_b, side_in.at[o - 1], chans, o))
        blk_copies[-1].start()
        blk_copies.append(across_blk(edge_b, edge_in.at[o - 1], chans + 1, o))
        blk_copies[-1].start()
    part = {}

    def products(those):
        for c, d in those:
            part[c, d] = jnp.sum(everyone[c] * everyone[d], axis=0, keepdims=True)

    everyone = list(shrunk)
    products([(c, d) for c in range(chans) for d in range(c, chans)])
    for copy in blk_copies:
        copy.wait_recv()
    brink = lax.broadcasted_iota(jnp.int32, (size - two, size), 1)
    brink = jnp.logical_or(brink < halo, brink >= size - halo)
    for o in range(1, nblk):
        sides = side_in[o - 1].astype(f32)
        for c in range(chans):
            edge = edge_in[o - 1, c].astype(f32)
            turned = pltpu.roll(sides, (2 * size - halo - c * two) % size, 1)
            middle = jnp.where(brink, turned, shr_in[o - 1, c].astype(f32))
            everyone.append(jnp.concatenate([edge[:halo], middle, edge[halo:]], axis=0))

    total = len(everyone)
    products([(c, d) for c in range(total) for d in range(max(c, chans), total)])
    gram = []
    for c in range(total):
        line = jnp.concatenate([part[min(c, d), max(c, d)] for d in range(total)], axis=0)
        gram.append(jnp.broadcast_to(jnp.sum(line, axis=1, keepdims=True), (total, size)))
    offset = weight_s[0] * float(size * size)
    subs = lax.broadcasted_iota(jnp.int32, (total, size), 0)
    lhs = [g + jnp.where(subs == c, offset, 0.0) for c, g in enumerate(gram)]
    rhs = list(gram)

    def column(x, k):
        return jnp.broadcast_to(x[k : k + 1, :], (total, size))

    for k in range(total):
        inv = 1.0 / column(lhs[k], k)
        lhs[k] = lhs[k] * inv
        rhs[k] = rhs[k] * inv
        for i in range(total):
            if i != k:
                factor = column(lhs[i], k)
                lhs[i] = lhs[i] - factor * lhs[k]
                rhs[i] = rhs[i] - factor * rhs[k]
    for d in range(chans):
        acc = None
        for c in range(total):
            term = rhs[c][d : d + 1, :] * everyone[c]
            acc = term if acc is None else acc + term
        out_ref[d] = acc

    for copy in oh_copies + row_copies + con_copies + blk_copies:
        copy.wait_send()
    for i, (dy, dx) in enumerate(corners()):

        @pl.when(near(dy, dx))
        def _():
            halo_copy(i, dy, dx).wait_send()


def body(
    nfy, nfx, nblk,
    sky_image, vis_data, interp_weights, tile_rows, facet_list, vis_count,
    wavelet_threshold, spectral_weight,
):
    chans, size, _ = sky_image.shape
    facets, tiles, slots, span = interp_weights.shape[2:6]
    left, right = dft_tables(size)
    levels = wavelet_threshold.shape[0]
    rows, parts = tiles * slots, 2 * chans
    flat = rows * parts
    halo = 2**levels
    rmat, cmat, beside, rim = smoothing_tables(size, halo, levels, chans)
    tall = size + 2 * halo
    vmem = pltpu.VMEM
    dma = pltpu.SemaphoreType.DMA
    any_spec = pl.BlockSpec(memory_space=pl.ANY)
    return pl.pallas_call(
        functools.partial(kernel, nfy, nfx, nblk, halo),
        out_shape=pltpu.VMEM((chans, size, size), f32),
        in_specs=[any_spec] * 14,
        out_specs=pl.BlockSpec(memory_space=pltpu.VMEM),
        scratch_shapes=[
            pltpu.SMEM(tile_rows.shape[:3] + (slots, tiles), jnp.int32),
            pltpu.SMEM(facet_list.shape, jnp.int32),
            pltpu.SMEM(vis_count.shape, jnp.int32),
            pltpu.SMEM(wavelet_threshold.shape, f32),
            pltpu.SMEM((1,), f32),
            vmem(sky_image.shape, bf16),
            vmem(vis_data.shape[2:], bf16),
            vmem(interp_weights.shape[2:], bf16),
            vmem(left.shape, bf16),
            vmem(right.shape, bf16),
            vmem(rmat.shape[1:], bf16),
            vmem(cmat.shape[1:], bf16),
            vmem(beside.shape, bf16),
            vmem(rim.shape, bf16),
            vmem((parts, vis_data.shape[4]), f32),
            vmem((nfx - 1, rows, size), f32),
            vmem((nfx, rows, size), f32),
            vmem((nfx * flat, size), f32),
            vmem((nfx - 1, flat, size), bf16),
            vmem((nfx, flat, size), bf16),
            vmem((nfx - 1, flat, size), bf16),
            vmem((nfx, flat, size), bf16),
            vmem((nfx * flat, size), f32),
            vmem((chans, size, size), bf16),
            vmem((size, size), bf16),
            vmem((size, size), bf16),
            vmem((chans, halo, size), bf16),
            vmem((chans, halo, size), bf16),
            vmem((tall, size), bf16),
            vmem((tall, size), bf16),
            vmem((chans, size - 2 * halo, size), bf16),
            vmem((nblk - 1, chans, size - 2 * halo, size), bf16),
            vmem((chans, 2 * halo, size), bf16),
            vmem((nblk - 1, chans, 2 * halo, size), bf16),
            vmem((size - 2 * halo, size), bf16),
            vmem((nblk - 1, size - 2 * halo, size), bf16),
            dma((9,)), dma((5,)),
            dma((nfx - 1,)), dma((nfx - 1,)),
            dma((nfx - 1,)), dma((nfx - 1,)),
            dma((nfx - 1,)), dma((nfx - 1,)),
            dma((8,)), dma((8,)),
            dma((nblk - 1, chans + 2)), dma((nblk - 1, chans + 2)),
        ],
        compiler_params=pltpu.CompilerParams(collective_id=0, has_side_effects=True),
    )(
        tile_rows.swapaxes(3, 4), facet_list, vis_count, wavelet_threshold, spectral_weight.reshape(1),
        sky_image, vis_data.reshape(vis_data.shape[2:]),
        interp_weights.reshape(interp_weights.shape[2:]), left, right,
        rmat, cmat, beside, rim,
    )


def solution(mesh):
    in_specs = (
        P("blk", "fy", "fx"),
        P("fy", "fx", "blk", None, None),
        P("fy", "fx", None, None, None, None, None),
        P("fy", "fx", None, None, None),
        P("fy", "fx", None),
        P("fy", "fx"),
        P(None, "blk"),
        P(),
    )
    out_specs = P("blk", "fy", "fx")
    step = functools.partial(body, mesh.shape["fy"], mesh.shape["fx"], mesh.shape["blk"])
    return jax.shard_map(step, mesh=mesh, in_specs=in_specs, out_specs=out_specs, check_vma=False)
```

```python
import functools
import math

import jax
import jax.numpy as jnp
import numpy as np
from jax import lax
from jax.experimental import pallas as pl
from jax.experimental.pallas import tpu as pltpu
from jax.sharding import PartitionSpec as P

MESH = pl.DeviceIdType.MESH
descent_step = 2.0
f32, bf16 = jnp.float32, jnp.bfloat16


def dft_tables(length):
    positions = np.arange(length)
    angles = (positions[:, None] * positions[None, :] % length) * (2.0 * math.pi / length)
    scaling = 1.0 / math.sqrt(length)
    cosine, sinus = np.cos(angles) * scaling, np.sin(angles) * scaling
    left = np.concatenate([cosine, -sinus], axis=0)
    right = np.concatenate(
        [np.concatenate([cosine, -sinus], axis=1), np.concatenate([sinus, cosine], axis=1)], axis=0
    )
    return jnp.asarray(left.astype(np.float32), bf16), jnp.asarray(right.astype(np.float32), bf16)


def smoothing_tables(size, halo, levels, chans):
    tall = size + 2 * halo
    gap = np.abs(np.arange(tall)[:, None] - np.arange(tall)[None, :])
    order = np.r_[halo:tall, 0:halo]
    row_all, col_all = [], []
    for before in (0, 1):
        for after in (0, 1):
            mask = np.r_[np.full(halo, before), np.ones(size), np.full(halo, after)]
            kept, lines = np.diag(mask), []
            for level in range(levels):
                smooth = 0.5 * (gap == 0) + 0.25 * (gap == 2**level)
                kept = mask[:, None] * (smooth @ kept)
                lines.append(kept[halo : halo + size][:, order])
            row_all.append(np.concatenate(lines, axis=0))
            col_all.append(np.concatenate([x[:, :size].T for x in lines], axis=1))
    beside = np.zeros((levels, size, chans, size))
    for level, x in enumerate(lines):
        for c in range(chans):
            beside[level, c * halo : (c + 1) * halo, c] = x[:, size : size + halo].T
            end = size - c * halo
            beside[level, end - halo : end, c] = x[:, size + halo :].T
    beside = beside.reshape(levels, size, chans * size)
    rim = np.concatenate([np.r_[x[:halo], x[size - halo :]][:, size:] for x in lines], axis=0)
    return [jnp.asarray(np.asarray(x, np.float32), bf16) for x in (row_all, col_all, beside, rim)]


def dot(a, b):
    return jnp.dot(a, b, preferred_element_type=f32)


def dot_nt(a, b):
    return lax.dot_general(a, b, (((1,), (1,)), ((), ())), preferred_element_type=f32)


def corners():
    return [(dy, dx) for dy in (-1, 0, 1) for dx in (-1, 0, 1) if (dy, dx) != (0, 0)]


def kernel(
    nfy, nfx, nblk, halo,
    rows_h, list_h, count_h, bound_h, weight_h, sky_h, vis_h, w_h, left_h, right_h, rmat_h, cmat_h, beside_h, rim_h,
    out_ref,
    rows_s, list_s, count_s, bound_s, weight_s,
    sky, vis, w, left, right, rmat, cmat, beside, rim, vis8,
    oh_out, oh_in, pick_f, row_out, row_in, con_out, con_in, con_f,
    step_b, pack_l, pack_r, land_t, land_b, land_l, land_r,
    shr_b, shr_in, edge_b, edge_in, side_b, side_in,
    load_sem, small_sem, oh_s, oh_r, row_s, row_r, con_s, con_r, halo_s, halo_r, blk_s, blk_r,
):
    fy, fx, bk = lax.axis_index("fy"), lax.axis_index("fx"), lax.axis_index("blk")
    _, _, facets, slots, tiles = rows_s.shape
    chans, size, _ = sky.shape
    rows = tiles * slots
    parts = 2 * chans

    small = [
        pltpu.make_async_copy(src, dst, small_sem.at[i])
        for i, (src, dst) in enumerate(
            [
                (rows_h, rows_s), (list_h, list_s), (count_h, count_s), (bound_h, bound_s),
                (weight_h, weight_s),
            ]
        )
    ]
    for load in small:
        load.start()

    for land in (land_t, land_b, land_l, land_r):
        land[...] = jnp.zeros(land.shape, bf16)

    has = {-1: {0: fy > 0, 1: fx > 0}, 1: {0: fy < nfy - 1, 1: fx < nfx - 1}}

    def near(dy, dx):
        cond = None
        for d, axis in ((dy, 0), (dx, 1)):
            if d:
                cond = has[d][axis] if cond is None else jnp.logical_and(cond, has[d][axis])
        return cond

    barrier = pltpu.get_barrier_semaphore()
    for o in range(1, nfx):
        pl.semaphore_signal(
            barrier, inc=1, device_id=(fy, lax.rem(fx + o, nfx), bk), device_id_type=MESH
        )
    for o in range(1, nblk):
        pl.semaphore_signal(
            barrier, inc=1, device_id=(fy, fx, lax.rem(bk + o, nblk)), device_id_type=MESH
        )
    for dy, dx in corners():
        if dy:

            @pl.when(near(dy, dx))
            def _():
                pl.semaphore_signal(
                    barrier, inc=1, device_id=(fy + dy, fx + dx, bk), device_id_type=MESH
                )

    def edges(at, count):
        return 2 * (at > 0).astype(jnp.int32) + (at < count - 1).astype(jnp.int32)

    loads = [
        pltpu.make_async_copy(src, dst, load_sem.at[i])
        for i, (src, dst) in enumerate(
            [
                (sky_h, sky), (left_h, left), (right_h, right), (vis_h, vis), (w_h, w),
                (rmat_h.at[edges(fy, nfy)], rmat), (cmat_h.at[edges(fx, nfx)], cmat),
                (beside_h, beside), (rim_h, rim),
            ]
        )
    ]
    for load in loads:
        load.start()

    for load in small:
        load.wait()

    sub = lax.broadcasted_iota(jnp.int32, (rows, size), 0)
    lane = lax.broadcasted_iota(jnp.int32, (rows, size), 1)
    hots = []
    for f in range(facets):
        wanted = jnp.zeros((rows, size), jnp.int32)
        for a in range(tiles):
            for n in range(slots):
                wanted = jnp.where(sub == a * slots + n, rows_s[0, 0, f, n, a], wanted)
        hots.append(jnp.where(wanted == lane, 1.0, 0.0))

    def match(f, o):
        return (list_s[0, 0, f] == lax.rem(fx + o, nfx)).astype(f32)

    for o in range(nfx):
        hot = hots[0] * match(0, o)
        for f in range(1, facets):
            hot = hot + hots[f] * match(f, o)
        if o:
            oh_out[o - 1] = hot
        else:
            oh_in[0] = hot

    waits = 0
    for v in ((fy > 0), (fy < nfy - 1)):
        waits = waits + v.astype(jnp.int32)
    sides = 1 + (fx > 0).astype(jnp.int32) + (fx < nfx - 1).astype(jnp.int32)
    pl.semaphore_wait(barrier, nfx - 1 + nblk - 1 + waits * sides)

    def peer(src, dst, send, recv, o, way):
        target = lax.rem(fx + o, nfx) if way > 0 else lax.rem(fx + nfx - o, nfx)
        return pltpu.make_async_remote_copy(
            src_ref=src, dst_ref=dst, send_sem=send.at[o - 1], recv_sem=recv.at[o - 1],
            device_id=(fy, target, bk), device_id_type=MESH,
        )

    def start_all(copies, way):
        low = fx < nfx // 2

        @pl.when(low if way > 0 else jnp.logical_not(low))
        def _():
            for copy in reversed(copies):
                copy.start()

        @pl.when(jnp.logical_not(low) if way > 0 else low)
        def _():
            for copy in copies:
                copy.start()

    oh_copies = [
        peer(oh_out.at[o - 1], oh_in.at[o], oh_s, oh_r, o, 1) for o in range(1, nfx)
    ]
    start_all(oh_copies, 1)

    for load in loads[:3]:
        load.wait()
    specs = []
    for c in range(chans):
        half = dot(left[...], sky[c]).astype(bf16)
        half = jnp.concatenate([half[:size], half[size:]], axis=1)
        specs.append(dot(half, right[...]).astype(bf16))

    for copy in oh_copies:
        copy.wait_recv()
    hot = oh_in[...].reshape(nfx * rows, size).astype(bf16)
    for c in range(chans):
        picked = dot(hot, specs[c])
        for p in range(2):
            pick_f[pl.ds(2 * c + p, nfx * rows, stride=parts), :] = picked[
                :, p * size : (p + 1) * size
            ]
    flat = rows * parts
    row_in[0] = pick_f[0:flat].astype(bf16)
    row_copies = []
    for o in range(1, nfx):
        row_out[o - 1] = pick_f[o * flat : (o + 1) * flat].astype(bf16)
    for o in range(1, nfx):
        row_copies.append(peer(row_out.at[o - 1], row_in.at[o], row_s, row_r, o, -1))
    start_all(row_copies, -1)

    adj = [
        dot_nt(left[p * size : (p + 1) * size], hot).astype(bf16) for p in range(2)
    ]
    for load in loads[3:]:
        load.wait()
    for c in range(chans):
        vis8[2 * c : 2 * c + 2, :] = vis[c].astype(f32)

    for copy in row_copies:
        copy.wait_recv()
    mine = []
    for f in range(facets):
        total = row_in[0].astype(f32) * match(f, 0)
        for o in range(1, nfx):
            total = total + row_in[o].astype(f32) * match(f, o)
        mine.append(total)
    live = count_s[0, 0]
    contrib = [[None] * rows for f in range(facets)]
    span = w.shape[3]
    for a in range(tiles):
        pred = -vis8[:, a * span : (a + 1) * span]
        for f in range(facets):
            for n in range(slots):
                at = a * slots + n
                row = mine[f][at * parts : (at + 1) * parts].astype(bf16)
                pred = pred + dot_nt(row, w[f, a, n])
        slot_id = lax.broadcasted_iota(jnp.int32, (parts, span), 1) + a * span
        residual = jnp.where(slot_id < live, pred, 0.0).astype(bf16)
        for f in range(facets):
            for n in range(slots):
                contrib[f][a * slots + n] = dot(residual, w[f, a, n])
    for o in range(nfx):
        for at in range(0, rows, 2):
            both = []
            for k in (at, at + 1):
                total = contrib[0][k] * match(0, o)
                for f in range(1, facets):
                    total = total + contrib[f][k] * match(f, o)
                both.append(total)
            value = jnp.concatenate(both, axis=0).astype(bf16)
            if o:
                con_out[o - 1, at * parts : (at + 2) * parts] = value
            else:
                con_in[0, at * parts : (at + 2) * parts] = value
    con_copies = []
    for o in range(1, nfx):
        con_copies.append(peer(con_out.at[o - 1], con_in.at[o], con_s, con_r, o, 1))
    start_all(con_copies, 1)
    for copy in con_copies:
        copy.wait_recv()

    con_f[...] = con_in[...].reshape(nfx * flat, size).astype(f32)
    halves = []
    for c in range(chans):
        grad = jnp.concatenate(
            [con_f[pl.ds(2 * c + p, nfx * rows, stride=parts), :] for p in range(2)], axis=1
        ).astype(bf16)
        halves.append(dot_nt(grad, right[...]).astype(bf16))
    stepped = []
    for c in range(chans):
        grad = dot(adj[0], halves[c][:, :size]) + dot(adj[1], halves[c][:, size:])
        stepped.append(sky[c].astype(f32) - descent_step * grad)

    lane1 = lax.broadcasted_iota(jnp.int32, (size, size), 1)
    seg_l = seg_r = None
    for c in range(chans):
        step_b[c] = stepped[c].astype(bf16)
        to_l = stepped[c] if c == 0 else pltpu.roll(stepped[c], c * halo, 1)
        to_r = stepped[c] if c == 0 else pltpu.roll(stepped[c], size - c * halo, 1)
        seg_l = to_l if c == 0 else jnp.where(lane1 >= c * halo, to_l, seg_l)
        seg_r = to_r if c == 0 else jnp.where(lane1 < size - c * halo, to_r, seg_r)
    mid = size // 2
    first = lane1[:mid] < mid
    pack_l[...] = jnp.where(first, seg_l[:mid], pltpu.roll(seg_l[mid:], mid, 1)).astype(bf16)
    pack_r[...] = jnp.where(first, pltpu.roll(seg_r[mid:], mid, 1), seg_r[:mid]).astype(bf16)
    sources = {
        -1: {-1: pack_l.at[0:halo], 0: step_b.at[:, 0:halo], 1: pack_r.at[0:halo]},
        0: {-1: pack_l, 1: pack_r},
        1: {
            -1: pack_l.at[mid - halo : mid],
            0: step_b.at[:, size - halo : size],
            1: pack_r.at[mid - halo : mid],
        },
    }
    spot = {0: slice(0, mid), -1: slice(mid, mid + halo), 1: slice(mid + halo, mid + 2 * halo)}

    def halo_copy(i, dy, dx):
        if dx == 0:
            dst = land_b if dy < 0 else land_t
        else:
            dst = (land_r if dx < 0 else land_l).at[spot[dy]]
        return pltpu.make_async_remote_copy(
            src_ref=sources[dy][dx], dst_ref=dst, send_sem=halo_s.at[i], recv_sem=halo_r.at[i],
            device_id=(fy + dy, fx + dx, bk), device_id_type=MESH,
        )

    for i, (dy, dx) in enumerate(corners()):

        @pl.when(near(dy, dx))
        def _():
            halo_copy(i, dy, dx).start()

    levels = bound_s.shape[0]
    inner = []
    for c in range(chans):
        if c % 2 == 0:
            pair = jnp.concatenate([step_b[d] for d in range(c, min(c + 2, chans))], axis=1)
            down = dot(rmat[:, :size], pair).astype(bf16)
        at = (c % 2) * size
        inner.append(
            [
                dot(
                    down[l * size : (l + 1) * size, at : at + size],
                    cmat[:, l * size : (l + 1) * size],
                )
                for l in range(levels)
            ]
        )

    def shrink(c, smooths):
        coarse, clipped = stepped[c], None
        for l, smooth in enumerate(smooths):
            bound = bound_s[l, c]
            detail = jnp.minimum(jnp.maximum(coarse - smooth, -bound), bound)
            clipped = detail if l == 0 else clipped + detail
            coarse = smooth
        return stepped[c] - clipped

    def across_blk(src, dst, i, o):
        return pltpu.make_async_remote_copy(
            src_ref=src, dst_ref=dst, send_sem=blk_s.at[o - 1, i], recv_sem=blk_r.at[o - 1, i],
            device_id=(fy, fx, lax.rem(bk + o, nblk)), device_id_type=MESH,
        )

    blk_copies = []
    for c in range(chans):
        shr_b[c] = shrink(c, inner[c])[halo : size - halo].astype(bf16)
        for o in range(1, nblk):
            blk_copies.append(across_blk(shr_b.at[c], shr_in.at[o - 1, c], c, o))
            blk_copies[-1].start()

    for i, (dy, dx) in enumerate(corners()):

        @pl.when(near(-dy, -dx))
        def _():
            halo_copy(i, dy, dx).wait_recv()

    side = lax.broadcasted_iota(jnp.int32, land_l.shape, 1) < mid
    at_r, at_l = land_r[...].astype(f32), land_l[...].astype(f32)
    upper = jnp.where(side, at_r, at_l)
    lower = pltpu.roll(jnp.where(side, at_l, at_r), mid, 1)
    packed = jnp.concatenate(
        [upper[:mid], lower[:mid], upper[mid : mid + halo], lower[mid + halo :]], axis=0
    ).astype(bf16)
    across = dot(rmat[...], packed).astype(bf16)
    from_beside = [
        dot(across[l * size : (l + 1) * size], beside[l]) for l in range(levels)
    ]
    margin = jnp.concatenate(
        [jnp.concatenate([land_b[c], land_t[c]], axis=0) for c in range(chans)], axis=1
    )
    margin = dot(rim[...], margin).astype(bf16)
    two = 2 * halo
    from_rim = [
        dot(
            jnp.concatenate(
                [
                    margin[l * two : (l + 1) * two, c * size : (c + 1) * size]
                    for c in range(chans)
                ],
                axis=0,
            ),
            cmat[:, l * size : (l + 1) * size],
        )
        for l in range(levels)
    ]
    shrunk = []
    for c in range(chans):
        smooths = []
        for l in range(levels):
            smooth = inner[c][l] + from_beside[l][:, c * size : (c + 1) * size]
            top = smooth[:halo] + from_rim[l][c * two : c * two + halo]
            bottom = smooth[size - halo :] + from_rim[l][c * two + halo : (c + 1) * two]
            smooths.append(jnp.concatenate([top, smooth[halo : size - halo], bottom], axis=0))
        value = shrink(c, smooths)
        shrunk.append(value)
        edge_b[c] = jnp.concatenate([value[:halo], value[size - halo :]], axis=0).astype(bf16)
        turned = pltpu.roll(value[halo : size - halo], (halo + c * two) % size, 1)
        sides = turned if c == 0 else jnp.where(lane1[: size - two] >= c * two, turned, sides)
    side_b[...] = sides.astype(bf16)
    for o in range(1, nblk):
        blk_copies.append(across_blk(side_b, side_in.at[o - 1], chans, o))
        blk_copies[-1].start()
        blk_copies.append(across_blk(edge_b, edge_in.at[o - 1], chans + 1, o))
        blk_copies[-1].start()
    part = {}

    def products(those):
        for c, d in those:
            part[c, d] = jnp.sum(everyone[c] * everyone[d], axis=0, keepdims=True)

    everyone = list(shrunk)
    products([(c, d) for c in range(chans) for d in range(c, chans)])
    for copy in blk_copies:
        copy.wait_recv()
    brink = lax.broadcasted_iota(jnp.int32, (size - two, size), 1)
    brink = jnp.logical_or(brink < halo, brink >= size - halo)
    for o in range(1, nblk):
        sides = side_in[o - 1].astype(f32)
        for c in range(chans):
            edge = edge_in[o - 1, c].astype(f32)
            turned = pltpu.roll(sides, (2 * size - halo - c * two) % size, 1)
            middle = jnp.where(brink, turned, shr_in[o - 1, c].astype(f32))
            everyone.append(jnp.concatenate([edge[:halo], middle, edge[halo:]], axis=0))

    total = len(everyone)
    products([(c, d) for c in range(total) for d in range(max(c, chans), total)])
    gram = []
    for c in range(total):
        line = jnp.concatenate([part[min(c, d), max(c, d)] for d in range(total)], axis=0)
        gram.append(jnp.broadcast_to(jnp.sum(line, axis=1, keepdims=True), (total, size)))
    offset = weight_s[0] * float(size * size)
    subs = lax.broadcasted_iota(jnp.int32, (total, size), 0)
    lhs = [g + jnp.where(subs == c, offset, 0.0) for c, g in enumerate(gram)]
    rhs = list(gram)

    def column(x, k):
        return jnp.broadcast_to(x[k : k + 1, :], (total, size))

    for k in range(total):
        inv = 1.0 / column(lhs[k], k)
        lhs[k] = lhs[k] * inv
        rhs[k] = rhs[k] * inv
        for i in range(total):
            if i != k:
                factor = column(lhs[i], k)
                lhs[i] = lhs[i] - factor * lhs[k]
                rhs[i] = rhs[i] - factor * rhs[k]
    for d in range(chans):
        acc = None
        for c in range(total):
            term = rhs[c][d : d + 1, :] * everyone[c]
            acc = term if acc is None else acc + term
        out_ref[d] = acc

    for copy in oh_copies + row_copies + con_copies + blk_copies:
        copy.wait_send()
    for i, (dy, dx) in enumerate(corners()):

        @pl.when(near(dy, dx))
        def _():
            halo_copy(i, dy, dx).wait_send()


def body(
    nfy, nfx, nblk,
    sky_image, vis_data, interp_weights, tile_rows, facet_list, vis_count,
    wavelet_threshold, spectral_weight,
):
    chans, size, _ = sky_image.shape
    facets, tiles, slots, span = interp_weights.shape[2:6]
    left, right = dft_tables(size)
    levels = wavelet_threshold.shape[0]
    rows, parts = tiles * slots, 2 * chans
    flat = rows * parts
    halo = 2**levels
    rmat, cmat, beside, rim = smoothing_tables(size, halo, levels, chans)
    tall = size + 2 * halo
    vmem = pltpu.VMEM
    dma = pltpu.SemaphoreType.DMA
    any_spec = pl.BlockSpec(memory_space=pl.ANY)
    return pl.pallas_call(
        functools.partial(kernel, nfy, nfx, nblk, halo),
        out_shape=pltpu.VMEM((chans, size, size), f32),
        in_specs=[any_spec] * 14,
        out_specs=pl.BlockSpec(memory_space=pltpu.VMEM),
        scratch_shapes=[
            pltpu.SMEM(tile_rows.shape[:3] + (slots, tiles), jnp.int32),
            pltpu.SMEM(facet_list.shape, jnp.int32),
            pltpu.SMEM(vis_count.shape, jnp.int32),
            pltpu.SMEM(wavelet_threshold.shape, f32),
            pltpu.SMEM((1,), f32),
            vmem(sky_image.shape, bf16),
            vmem(vis_data.shape[2:], bf16),
            vmem(interp_weights.shape[2:], bf16),
            vmem(left.shape, bf16),
            vmem(right.shape, bf16),
            vmem(rmat.shape[1:], bf16),
            vmem(cmat.shape[1:], bf16),
            vmem(beside.shape, bf16),
            vmem(rim.shape, bf16),
            vmem((parts, vis_data.shape[4]), f32),
            vmem((nfx - 1, rows, size), f32),
            vmem((nfx, rows, size), f32),
            vmem((nfx * flat, size), f32),
            vmem((nfx - 1, flat, size), bf16),
            vmem((nfx, flat, size), bf16),
            vmem((nfx - 1, flat, size), bf16),
            vmem((nfx, flat, size), bf16),
            vmem((nfx * flat, size), f32),
            vmem((chans, size, size), bf16),
            vmem((size // 2, size), bf16),
            vmem((size // 2, size), bf16),
            vmem((chans, halo, size), bf16),
            vmem((chans, halo, size), bf16),
            vmem((tall - size // 2, size), bf16),
            vmem((tall - size // 2, size), bf16),
            vmem((chans, size - 2 * halo, size), bf16),
            vmem((nblk - 1, chans, size - 2 * halo, size), bf16),
            vmem((chans, 2 * halo, size), bf16),
            vmem((nblk - 1, chans, 2 * halo, size), bf16),
            vmem((size - 2 * halo, size), bf16),
            vmem((nblk - 1, size - 2 * halo, size), bf16),
            dma((9,)), dma((5,)),
            dma((nfx - 1,)), dma((nfx - 1,)),
            dma((nfx - 1,)), dma((nfx - 1,)),
            dma((nfx - 1,)), dma((nfx - 1,)),
            dma((8,)), dma((8,)),
            dma((nblk - 1, chans + 2)), dma((nblk - 1, chans + 2)),
        ],
        compiler_params=pltpu.CompilerParams(collective_id=0, has_side_effects=True),
    )(
        tile_rows.swapaxes(3, 4), facet_list, vis_count, wavelet_threshold, spectral_weight.reshape(1),
        sky_image, vis_data.reshape(vis_data.shape[2:]),
        interp_weights.reshape(interp_weights.shape[2:]), left, right,
        rmat, cmat, beside, rim,
    )


def solution(mesh):
    in_specs = (
        P("blk", "fy", "fx"),
        P("fy", "fx", "blk", None, None),
        P("fy", "fx", None, None, None, None, None),
        P("fy", "fx", None, None, None),
        P("fy", "fx", None),
        P("fy", "fx"),
        P(None, "blk"),
        P(),
    )
    out_specs = P("blk", "fy", "fx")
    step = functools.partial(body, mesh.shape["fy"], mesh.shape["fx"], mesh.shape["blk"])
    return jax.shard_map(step, mesh=mesh, in_specs=in_specs, out_specs=out_specs, check_vma=False)
```
